32 devices in a mesh: gx: 8 (over y, x, core), gy: 4 (over z).
Axes of the slice: x: 2, y: 2, z: 4, core: 2. Of those that a mesh axis runs over, the one named last changes fastest.
Arguments:
- rhs_conc: float32 [16, 64, 2048], P('gx', 'gy'), may hold values from -60 to 60
- rhs_pots: float32 [16, 64, 33], P('gx', 'gy'), may hold values from -60 to 60
- diffusion: float32 [16, 64, 32], P('gx', 'gy'), may hold values from 0.05 to 5
- exchange: float32 [16, 64, 32], P('gx', 'gy'), may hold values from 0.2 to 4
- slope: float32 [16, 64, 32], P('gx', 'gy'), may hold values from 0.1 to 1
Outputs:
- sol_conc: float32 [16, 64, 2048], P('gx', 'gy')
- sol_pots: float32 [16, 64, 33], P('gx', 'gy')
The draws below stay inside these ranges and needn't reach their ends.
All inputs are finite; a program needn't handle non-finite values.
Results may differ from the reference program's by a relative error of at most 0.0003.
Values sent between devices are 32-bit elements; how exact they have to be, the bound alone decides.
A program may use at most 64 MiB of HBM per device.

```python
import math
import jax
import jax.numpy as jnp
from jax import lax

NE = 32
NR = 64
ITERS = 10
NX = 16
NY = 64


def column_scale(key):
    scale_key = jax.random.fold_in(key, 7)
    row_place = jnp.arange(NX, dtype=jnp.float32)[:, None] / max(NX - 1, 1)
    spread_field = jnp.exp(jax.random.uniform(scale_key, (NX, NY), jnp.float32) * math.log(10.0))
    scale_field = spread_field * jnp.exp(row_place * math.log(3.0))
    return 0.25 * scale_field


def draw_values(key, width):
    values = jnp.clip(jax.random.normal(key, (NX, NY, width), jnp.float32), -5.0, 5.0)
    return values


def draw_rhs_conc(key, part):
    scale_field = column_scale(key)
    values = draw_values(jax.random.fold_in(key, 11), NE * NR)
    return scale_field[:, :, None] * values


def draw_rhs_pots(key, part):
    scale_field = column_scale(key)
    values = draw_values(jax.random.fold_in(key, 13), NE + 1)
    return scale_field[:, :, None] * values


def levels(stream_key, extent, cuts, low, high):
    def one(position, blocks):
        heights = jax.random.uniform(jax.random.fold_in(jax.random.fold_in(stream_key, 6), position), (blocks,), jnp.float32, low / len(cuts), high / len(cuts))
        return jnp.repeat(jnp.exp(heights), extent[position] // blocks).reshape((-1,) + (1,) * (len(extent) - position - 1))

    gain = one(*cuts[0])
    for cut in cuts[1:]:
        gain = gain * one(*cut)
    return gain


def setup_inputs(seed: int = 0) -> dict:
    seeds = jax.random.split(jax.random.key(seed), 6)
    rhs_conc = draw_rhs_conc(jax.random.fold_in(seeds[5], 71), 0)
    rhs_pots = draw_rhs_pots(jax.random.fold_in(seeds[5], 71), 0)
    diffusion = jnp.clip(jnp.exp(math.log(5.0) - 4.6051702 * jax.random.uniform(seeds[2], (NX, NY, NE), jnp.float32) ** levels(seeds[2], (NX, NY, NE), ((0, 8), (1, 4)), -0.2, 0.2)), 0.05, 5.0)
    exchange = jnp.clip(jnp.exp(math.log(4.0) - 2.9957323 * jax.random.uniform(seeds[3], (NX, NY, NE), jnp.float32) ** levels(seeds[3], (NX, NY, NE), ((0, 8), (1, 4)), -0.2, 0.2)), 0.2, 4.0)
    slope = jnp.clip(0.1 + 0.9 * jax.random.uniform(seeds[4], (NX, NY, NE), jnp.float32) ** levels(seeds[4], (NX, NY, NE), ((0, 8), (1, 4)), -0.2, 0.2), 0.1, 1.0)
    return dict(rhs_conc=rhs_conc, rhs_pots=rhs_pots, diffusion=diffusion, exchange=exchange, slope=slope)


node_cond = 1.0
plane_cond = 0.5
collector_cond = 2.0
epsilon = 1e-06

def mirror_laplace(values):
    inner = jnp.concatenate([values[..., :1], values[..., :-1]], axis=-1)
    outer = jnp.concatenate([values[..., 1:], values[..., -1:]], axis=-1)
    return 2.0 * values - inner - outer

def local_operator(conc, padded, diffusion, exchange, slope):
    nodes = exchange.shape[2]
    shell_count = conc.shape[2] // nodes
    shells = conc.reshape(conc.shape[0], conc.shape[1], nodes, shell_count)
    center = padded[1:-1, 1:-1]
    lateral = 4.0 * center - padded[2:, 1:-1] - padded[:-2, 1:-1] - padded[1:-1, 2:] - padded[1:-1, :-2]
    node_pot = center[..., :nodes]
    collector = center[..., nodes]
    current = exchange * (node_pot - collector[..., None])
    surface = shells[..., shell_count - 1]
    surface_flag = (lax.broadcasted_iota(jnp.int32, (shell_count,), 0) == shell_count - 1).astype(jnp.float32)
    new_shells = shells + diffusion[..., None] * mirror_laplace(shells) + current[..., None] * surface_flag
    new_nodes = node_cond * mirror_laplace(node_pot) + current - slope * surface + plane_cond * lateral[..., :nodes]
    new_collector = collector_cond * lateral[..., nodes] - lax.optimization_barrier(jnp.mean(current, axis=-1))
    return (new_shells.reshape(conc.shape), jnp.concatenate([new_nodes, new_collector[..., None]], axis=-1))

def least_squares(columns, start_norm):
    count = len(columns)
    target = [start_norm] + [jnp.zeros_like(start_norm) for step in range(count)]
    cosines = []
    sines = []
    upper_rows = []
    for step in range(count):
        entries = list(columns[step])
        for row in range(step):
            first = cosines[row] * entries[row] + sines[row] * entries[row + 1]
            second = cosines[row] * entries[row + 1] - sines[row] * entries[row]
            entries[row] = first
            entries[row + 1] = second
        radius = jnp.sqrt(entries[step] * entries[step] + entries[step + 1] * entries[step + 1])
        cosine = entries[step] / radius
        sine = entries[step + 1] / radius
        entries[step] = radius
        cosines.append(cosine)
        sines.append(sine)
        lead = target[step]
        target[step] = cosine * lead
        target[step + 1] = -sine * lead
        upper_rows.append(entries[:step + 1])
    weights = [None] * count
    for row in range(count - 1, -1, -1):
        total = target[row]
        for later in range(row + 1, count):
            total = total - upper_rows[later][row] * weights[later]
        weights[row] = total / upper_rows[row][row]
    return weights

def apply_operator(conc, pots, diffusion, exchange, slope):
    padded = jnp.pad(pots, ((1, 1), (1, 1), (0, 0)))
    return local_operator(conc, padded, diffusion, exchange, slope)

def reference(rhs_conc, rhs_pots, diffusion, exchange, slope):
    start_norm = jnp.sqrt(jnp.sum(rhs_conc * rhs_conc) + jnp.sum(rhs_pots * rhs_pots) + epsilon)
    basis = [(rhs_conc / start_norm, rhs_pots / start_norm)]
    columns = []
    for step in range(ITERS):
        image_conc, image_pots = apply_operator(basis[step][0], basis[step][1], diffusion, exchange, slope)
        coeffs = [jnp.sum(vector[0] * image_conc) + jnp.sum(vector[1] * image_pots) for vector in basis]
        rest_conc, rest_pots = (image_conc, image_pots)
        for row in range(step + 1):
            rest_conc = rest_conc - coeffs[row] * basis[row][0]
            rest_pots = rest_pots - coeffs[row] * basis[row][1]
        height = jnp.sqrt(jnp.sum(rest_conc * rest_conc) + jnp.sum(rest_pots * rest_pots) + epsilon)
        basis.append((rest_conc / height, rest_pots / height))
        columns.append(coeffs + [height])
    weights = least_squares(columns, start_norm)
    sol_conc = weights[0] * basis[0][0]
    sol_pots = weights[0] * basis[0][1]
    for step in range(1, ITERS):
        sol_conc = sol_conc + weights[step] * basis[step][0]
        sol_pots = sol_pots + weights[step] * basis[step][1]
    return (sol_conc, sol_pots)
```

```python
import functools

import jax
import jax.numpy as jnp
from jax import lax
from jax.experimental import pallas as pl
from jax.experimental.pallas import tpu as pltpu
from jax.sharding import PartitionSpec as P

ITERS = 10
LANES = 128
CHUNK = 16
PLAN = (2, 2, 2, 2, 2)
ADAPTIVE = 2

node_cond = 1.0
plane_cond = 0.5
collector_cond = 2.0
epsilon = 1e-06
center = 10.0
radius = 10.0
least_height = 0.05
least_pivot = 3e-07
MESH = pl.DeviceIdType.MESH


def add(terms):
    terms = [t for t in terms if t is not None]
    while len(terms) > 1:
        pairs = [terms[k] + terms[k + 1] for k in range(0, len(terms) - 1, 2)]
        terms = pairs + ([terms[-1]] if len(terms) % 2 else [])
    return terms[0]


def factor(gram):
    size = len(gram)
    left = [[gram[i][j] for j in range(size)] for i in range(size)]
    upper = [[None] * size for _ in range(size)]
    inverse = []
    for k in range(size):
        pivot = left[k][k]
        good = pivot > least_pivot * gram[k][k]
        inv = jnp.where(good, lax.rsqrt(jnp.where(good, pivot, 1.0)), 0.0)
        inverse.append(inv)
        upper[k][k] = pivot * inv
        for j in range(k + 1, size):
            upper[k][j] = left[k][j] * inv
        for i in range(k + 1, size):
            for j in range(i, size):
                left[i][j] = left[i][j] - upper[k][i] * upper[k][j]
    return upper, inverse


def project(upper, inverse, recurrence):
    columns = []
    for k, (alpha, gamma, beta) in enumerate(recurrence):
        column = []
        for i in range(k + 2):
            terms = [beta * upper[i][k + 1]]
            if i <= k:
                terms.append(alpha * upper[i][k])
            if i <= k - 1 and gamma is not None:
                terms.append(gamma * upper[i][k - 1])
            value = add(terms)
            known = [columns[m][i] * upper[m][k] for m in range(max(i - 1, 0), k)]
            if known:
                value = value - add(known)
            column.append(value * inverse[k])
        columns.append(column)
    return columns


def arnoldi(upper, inverse, images, count):
    height = jnp.sqrt(upper[0][0] * upper[0][0] + epsilon)
    start = height
    vectors = [[upper[0][0] / height]]
    columns = []
    for j in range(count):
        newest = vectors[j]
        image = [
            add([images[k][t] * newest[k] for k in range(max(t - 1, 0), j + 1)])
            for t in range(j + 2)
        ]
        coeffs = [
            add([vectors[i][t] * image[t] for t in range(i + 1)]) for i in range(j + 1)
        ]
        rest = [
            image[t] - add([coeffs[i] * vectors[i][t] for i in range(t, j + 1)])
            for t in range(j + 1)
        ] + [image[j + 1]]
        height = jnp.sqrt(add([r * r for r in rest]) + epsilon)
        columns.append(coeffs + [height])
        if j + 1 < count:
            scale = 1.0 / height
            vectors.append([r * scale for r in rest])
    return start, vectors, columns


def least_squares(columns, start):
    target, cosines, sines, uppers = [start], [], [], []
    for step, column in enumerate(columns):
        entries = list(column)
        for row in range(step):
            first = cosines[row] * entries[row] + sines[row] * entries[row + 1]
            second = cosines[row] * entries[row + 1] - sines[row] * entries[row]
            entries[row] = first
            entries[row + 1] = second
        size = jnp.sqrt(entries[step] * entries[step] + entries[step + 1] * entries[step + 1])
        shrink = 1.0 / size
        cosine = entries[step] * shrink
        sine = entries[step + 1] * shrink
        entries[step] = size
        cosines.append(cosine)
        sines.append(sine)
        lead = target[step]
        target[step] = cosine * lead
        target.append(-sine * lead)
        uppers.append((entries[: step + 1], shrink))
    weights = [None] * len(columns)
    for row in range(len(columns) - 1, -1, -1):
        total = target[row]
        for later in range(len(columns) - 1, row, -1):
            total = total - uppers[later][0][row] * weights[later]
        weights[row] = total * uppers[row][1]
    return weights


def expand(weights, vectors, upper, inverse):
    count = len(weights)
    along = [add([vectors[j][t] * weights[j] for j in range(t, count)]) for t in range(count)]
    out = [None] * count
    for row in range(count - 1, -1, -1):
        total = along[row]
        for later in range(count - 1, row, -1):
            total = total - upper[row][later] * out[later]
        out[row] = total * inverse[row]
    return out


def surroundings(cx, cy, depth):
    def away(extent, offset):
        return (abs(offset) - 1) * extent + 1 if offset else 0

    found = {}
    for a in range(-depth, depth + 1):
        for b in range(-depth, depth + 1):
            distance = away(cx, a) + away(cy, b)
            if 0 < distance <= depth:
                found[a, b] = distance
    return found


def cycle(
    sizes,
    conc_ref,
    pots_ref,
    diff_ref,
    exch_ref,
    slope_ref,
    sol_conc_ref,
    sol_pots_ref,
    turned,
    basis,
    raw_pots,
    raw_fixed,
    sent,
    halos,
    fixed_sent,
    fixed_halos,
    rows,
    sent_rows,
    edge_send,
    edge_recv,
    fixed_send,
    fixed_recv,
    row_send,
    row_recv,
    load_sem,
    small_sem,
    out_sem,
):
    nx, ny = sizes
    count = nx * ny
    cx, cy = conc_ref.shape[0], conc_ref.shape[1]
    cells = cx * cy
    nodes = exch_ref.shape[2]
    shells = conc_ref.shape[2] // nodes
    groups = LANES // cells
    subs = nodes // groups
    mx = lax.axis_index("gx")
    my = lax.axis_index("gy")
    me = mx * ny + my
    deepest = max(PLAN)
    around = surroundings(cx, cy, deepest)
    order = sorted(around, key=lambda o: -around[o])
    place = {o: i for i, o in enumerate(order)}

    def peers(act):
        if count <= 32:
            for dx in range(nx - 1, -1, -1):
                for dy in range(ny - 1, -1, -1):
                    if dx or dy:
                        act(lax.rem(mx + dx, nx), lax.rem(my + dy, ny))
        else:

            def one(p, carry):
                other = lax.rem(me + p, count)
                act(lax.div(other, ny), lax.rem(other, ny))
                return carry

            lax.fori_loop(1, count, one, 0)

    barrier = pltpu.get_barrier_semaphore()
    peers(
        lambda px, py: pl.semaphore_signal(
            barrier, inc=1, device_id={"gx": px, "gy": py}, device_id_type=MESH
        )
    )

    span = subs * shells
    loads = []
    for x in range(cx):
        for g in range(groups):
            edge_row = g * cells + x * cy
            loads.append(
                pltpu.make_async_copy(
                    conc_ref.at[x, :, g * span : (g + 1) * span],
                    turned.at[edge_row : edge_row + cy, :],
                    load_sem.at[x, g],
                )
            )
    small = [pltpu.make_async_copy(pots_ref, raw_pots, small_sem.at[0])]
    for k, ref in enumerate((exch_ref, slope_ref, diff_ref)):
        small.append(pltpu.make_async_copy(ref, raw_fixed.at[k], small_sem.at[k + 1]))
    for copy in small + loads:
        copy.start()
    for copy in small:
        copy.wait()

    def fold_nodes(block):
        return block.reshape(cells, block.shape[2]).T

    def node_register(flat_t):
        return jnp.concatenate(
            [flat_t[g * subs : (g + 1) * subs, :] for g in range(groups)], axis=1
        )

    exch = node_register(fold_nodes(raw_fixed[0]))
    slope = node_register(fold_nodes(raw_fixed[1]))
    diff = node_register(fold_nodes(raw_fixed[2]))
    pots_t = fold_nodes(raw_pots[...])
    pot = node_register(pots_t)
    vol_row = pots_t[nodes : nodes + 1, :]
    vol = jnp.broadcast_to(jnp.concatenate([vol_row] * groups, axis=1), (subs, LANES))
    for k, value in enumerate((exch, slope, diff)):
        fixed_sent[k] = value

    lane = lax.broadcasted_iota(jnp.int32, (subs, LANES), 1)
    sub = lax.broadcasted_iota(jnp.int32, (subs, LANES), 0)
    group = lane // cells
    cell = lane % cells
    cell_x = cell // cy
    cell_y = cell % cy
    single = ((sub == 0) & (group == 0)).astype(jnp.float32)
    first_sub, last_sub = sub == 0, sub == subs - 1
    first_group, last_group = group == 0, group == groups - 1
    low_x, high_x = cell_x == 0, cell_x == cx - 1
    low_y, high_y = cell_y == 0, cell_y == cy - 1
    zero = jnp.zeros((subs, LANES), jnp.float32)

    there = {}
    for a, b in order:
        there[a, b] = (
            (mx + a >= 0) & (mx + a < nx) & (my + b >= 0) & (my + b < ny)
        )

    def roll(value, shift, axis=1):
        shift = shift % value.shape[axis]
        return pltpu.roll(value, shift, axis) if shift else value

    def sides(p, low_block, high_block, edge_low, edge_high, step, wide):
        low = roll(p, step)
        low = jnp.where(edge_low, zero if low_block is None else roll(low_block, -wide), low)
        high = roll(p, -step)
        high = jnp.where(edge_high, zero if high_block is None else roll(high_block, wide), high)
        return low + high

    def plane(p, near, member):
        def at(offset):
            return None if near[offset] is None else near[offset][member]

        across = sides(p, at((-1, 0)), at((1, 0)), low_x, high_x, cy, (cx - 1) * cy)
        along = sides(p, at((0, -1)), at((0, 1)), low_y, high_y, 1, cy - 1)
        return 4.0 * p - (across + along)

    def node_mirror(p):
        low = roll(p, 1, 0)
        inner = jnp.where(first_sub, jnp.where(first_group, p, roll(low, cells)), low)
        high = roll(p, -1, 0)
        outer = jnp.where(last_sub, jnp.where(last_group, p, roll(high, -cells)), high)
        return 2.0 * p - inner - outer

    def node_mean(value):
        total = jnp.broadcast_to(jnp.sum(value, axis=0, keepdims=True), (subs, LANES))
        parts = [total] + [roll(total, g * cells) for g in range(1, groups)]
        return add(parts) * (1.0 / nodes)

    nowhere = {(-1, 0): None, (1, 0): None, (0, -1): None, (0, 1): None}

    def pots_image(field, near, surface, fixed):
        p, v = field
        current = fixed[0] * (p - v)
        new_p = (
            node_cond * node_mirror(p)
            + current
            - fixed[1] * surface
            + plane_cond * plane(p, near, 0)
        )
        new_v = collector_cond * plane(v, near, 1) - node_mean(current)
        return new_p, new_v, current

    def relate(image, here, before, terms):
        alpha, gamma, _, inverse = terms
        value = image - alpha * here
        if gamma is not None:
            value = value - gamma * before
        return value * inverse

    def shell_images(levels, before, current, diffusion, terms):
        out = []
        for k in range(len(levels) - 1):
            here = levels[k]
            image = here + diffusion * (
                here - levels[k + 1] if k == 0 else 2.0 * here - levels[k - 1] - levels[k + 1]
            )
            if k == 0:
                image = image + current
            out.append(relate(image, here, before[k] if before else None, terms))
        return out

    def full_image(k, current, terms, fields, source=None, target=None):
        alpha, gamma, _, inverse = terms
        keep = (1.0 - alpha) * inverse
        spread = diff * inverse
        middle = (keep + 2.0 * spread)[None]
        spread = spread[None]
        basis[k, 0] = basis[k, 1]
        basis[k, shells + 1] = basis[k, shells]
        newest = fields[k + 1]
        starts = [
            fields[i][0] * newest[0] + fields[i][1] * (newest[1] * single) for i in range(k + 2)
        ]
        pushed = inverse * current

        def part(at, carry, last):
            here = basis[k, pl.ds(at + 1, CHUNK)]
            low = basis[k, pl.ds(at, CHUNK)]
            high = basis[k, pl.ds(at + 2, CHUNK)]
            new = middle * here - spread * (low + high)
            if gamma is not None:
                new = new - (gamma * inverse) * basis[k - 1, pl.ds(at + 1, CHUNK)]
            if last:
                new = jnp.concatenate([new[:-1], new[-1:] + pushed[None]], axis=0)
            basis[k + 1, pl.ds(at + 1, CHUNK)] = new
            others = [basis[i, pl.ds(at + 1, CHUNK)] for i in range(k)] + [here, new]
            return tuple(c + jnp.sum(o * new, axis=0) for c, o in zip(carry, others))

        parts = shells // CHUNK
        carry = lax.fori_loop(
            0, parts - 1, lambda c, carry: part(c * CHUNK, carry, False), tuple(starts)
        )
        return list(part((parts - 1) * CHUNK, carry, True))

    def line_up(products, offset):
        padded = -(-len(products) // 8) * 8
        stacked = [jnp.sum(d, axis=0, keepdims=True) for d in products]
        stacked += [zero[:1]] * (padded - len(products))
        tall = jnp.sum(jnp.concatenate(stacked, axis=0), axis=1, keepdims=True)
        at_row = lax.broadcasted_iota(jnp.int32, (padded, LANES), 0) + offset
        at_lane = lax.broadcasted_iota(jnp.int32, (padded, LANES), 1)
        return jnp.sum(jnp.where(at_row == at_lane, tall, 0.0), axis=0, keepdims=True)

    def row_copy(step, px, py):
        return pltpu.make_async_remote_copy(
            src_ref=sent_rows.at[step],
            dst_ref=rows.at[step, me],
            send_sem=row_send.at[step],
            recv_sem=row_recv.at[step],
            device_id={"gx": px, "gy": py},
            device_id_type=MESH,
        )

    def send_row(step, row):
        sent_rows[step] = row
        rows[step, me] = row
        peers(lambda px, py: row_copy(step, px, py).start())

    def take_row(step, wanted):
        part = rows.at[step, pl.ds(0, count - 1)]
        pltpu.make_async_copy(part, part, row_recv.at[step]).wait()
        total = jnp.sum(rows[step], axis=0)
        return [jnp.broadcast_to(total[:, k : k + 1], (subs, LANES)) for k in range(wanted)]

    def copies_of(phase):
        depth = PLAN[phase]
        out = []
        for o in order:
            if around[o] > depth:
                continue
            a, b = o
            items = 2 + depth - around[o]
            out.append(
                (
                    o,
                    pltpu.make_async_remote_copy(
                        src_ref=sent.at[phase, pl.ds(0, items)],
                        dst_ref=halos.at[phase, place[-a, -b], pl.ds(0, items)],
                        send_sem=edge_send.at[phase, place[o]],
                        recv_sem=edge_recv.at[phase, place[-a, -b]],
                        device_id={
                            "gx": lax.rem(mx + a + nx * deepest, nx),
                            "gy": lax.rem(my + b + ny * deepest, ny),
                        },
                        device_id_type=MESH,
                    ),
                )
            )
        return out

    def arrivals_of(phase):
        depth = PLAN[phase]
        out = []
        for o in order:
            if around[o] > depth:
                continue
            items = 2 + depth - around[o]
            part = halos.at[phase, place[o], pl.ds(0, items)]
            out.append((o, pltpu.make_async_copy(part, part, edge_recv.at[phase, place[o]])))
        return out

    def fixed_copies():
        out = []
        for o in order:
            if around[o] > deepest - 1:
                continue
            a, b = o
            items = 3 if around[o] <= deepest - 2 else 2
            part = fixed_halos.at[place[o], pl.ds(0, items)]
            out.append(
                (
                    o,
                    pltpu.make_async_remote_copy(
                        src_ref=fixed_sent.at[pl.ds(0, items)],
                        dst_ref=fixed_halos.at[place[-a, -b], pl.ds(0, items)],
                        send_sem=fixed_send.at[place[o]],
                        recv_sem=fixed_recv.at[place[-a, -b]],
                        device_id={
                            "gx": lax.rem(mx + a + nx * deepest, nx),
                            "gy": lax.rem(my + b + ny * deepest, ny),
                        },
                        device_id_type=MESH,
                    ),
                    pltpu.make_async_copy(part, part, fixed_recv.at[place[o]]),
                )
            )
        return out

    def send_edges(phase, field, levels):
        sent[phase, 0] = field[0]
        sent[phase, 1] = field[1]
        for k, level in enumerate(levels):
            sent[phase, 2 + k] = level
        for o, copy in copies_of(phase):
            pl.when(there[o])(copy.start)

    def tops(k, number):
        return [basis[k, shells - j] for j in range(number)]

    for copy in loads:
        copy.wait()
    turned_t = turned[...].T.reshape(subs, shells, LANES)
    for s in range(subs):
        basis[0, 1 : shells + 1, s, :] = turned_t[s]

    fields = [(pot, vol)] + [None] * ITERS
    fixed_own = (exch, slope)
    guess = [(center, None, radius, 1.0 / radius), (center, radius / 2, radius / 2, 2.0 / radius)]

    pl.semaphore_wait(barrier, count - 1)
    send_edges(0, fields[0], tops(0, PLAN[0] - 1))
    fixed_moves = fixed_copies()
    for o, copy, _ in fixed_moves:
        pl.when(there[o])(copy.start)

    local = [fields[0]]
    products = [
        pot * pot
        + vol * (vol * single)
        + lax.fori_loop(
            0,
            shells // CHUNK,
            lambda c, t: t
            + jnp.sum(
                basis[0, pl.ds(c * CHUNK + 1, CHUNK)] * basis[0, pl.ds(c * CHUNK + 1, CHUNK)],
                axis=0,
            ),
            zero,
        )
    ]
    first_square = products[0]
    for k in range(ADAPTIVE):
        new_p, new_v, current = pots_image(local[k], nowhere, basis[k, shells], fixed_own)
        before = local[k - 1] if k else (None, None)
        local.append(
            (
                relate(new_p, local[k][0], before[0], guess[k]),
                relate(new_v, local[k][1], before[1], guess[k]),
            )
        )
        products += full_image(k, current, guess[k], local)
    send_row(0, line_up(products, 0))

    def symmetric(sums, size):
        gram = [[None] * size for _ in range(size)]
        at = 0
        for j in range(size):
            for i in range(j + 1):
                gram[i][j] = gram[j][i] = sums[at]
                at += 1
        return gram

    def lanczos(sums):
        upper, inverse = factor(symmetric(sums, ADAPTIVE + 1))
        columns = project(upper, inverse, [(a, g, b) for a, g, b, _ in guess])
        out = []
        for k in range(ADAPTIVE):
            height = jnp.maximum(columns[k][k + 1], least_height)
            gamma = columns[k][k - 1] if k else None
            out.append((columns[k][k], gamma, height, 1.0 / height))
        return out

    recurrence = None
    row = line_up([first_square], 0)
    at = 1
    k = 0
    earlier = {}
    for phase, depth in enumerate(PLAN):
        more = phase + 1 < len(PLAN)
        ahead = PLAN[phase + 1] - 1 if more else 0
        if phase == 0:
            recurrence = lanczos(take_row(0, len(products)))
        for step in range(depth):
            if k + step < ADAPTIVE:
                continue
            gamma = radius / 2 if step or depth <= 2 else None
            recurrence.append((center, gamma, radius / 2, 2.0 / radius))
        for o, copy in arrivals_of(phase):
            pl.when(there[o])(copy.wait)
        if phase == 0:
            fixed = {(0, 0): (exch, slope, diff)}
            for o, _, wait in fixed_moves:
                pl.when(there[o])(wait.wait)
            for o, _, _ in fixed_moves:
                fixed[o] = tuple(
                    jnp.where(there[o], fixed_halos[place[o], i], 0.0)
                    for i in range(3 if around[o] <= deepest - 2 else 2)
                )
        now = {(0, 0): fields[k]}
        levels = {(0, 0): tops(k, depth + ahead)}
        before = {(0, 0): tops(k - 1, depth + ahead - 1) if k else None}
        for o in order:
            if around[o] <= depth:
                now[o] = tuple(
                    jnp.where(there[o], halos[phase, place[o], i], 0.0) for i in range(2)
                )
                levels[o] = [
                    jnp.where(there[o], halos[phase, place[o], 2 + i], 0.0)
                    for i in range(depth - around[o])
                ]
                before[o] = None
        currents = []
        past = earlier
        if k:
            past = dict(earlier)
            past[0, 0] = fields[k - 1]
        for step in range(depth):
            terms = recurrence[k + step]
            reach = depth - step - 1
            new, new_levels = {}, {}
            for o in now:
                if o != (0, 0) and around[o] > reach:
                    continue
                near = {
                    side: now.get((o[0] + side[0], o[1] + side[1])) for side in nowhere
                }
                new_p, new_v, current = pots_image(now[o], near, levels[o][0], fixed[o])
                last = past.get(o, (None, None))
                p = relate(new_p, now[o][0], last[0], terms)
                v = relate(new_v, now[o][1], last[1], terms)
                if o != (0, 0):
                    p = jnp.where(there[o], p, 0.0)
                    v = jnp.where(there[o], v, 0.0)
                else:
                    currents.append(current)
                new[o] = (p, v)
                if len(levels[o]) > 1:
                    new_levels[o] = shell_images(
                        levels[o], before[o], current, fixed[o][2], terms
                    )
                else:
                    new_levels[o] = []
            past, now = now, new
            before, levels = levels, new_levels
            fields[k + step + 1] = now[0, 0]
        earlier = {o: f for o, f in past.items() if o != (0, 0)}
        if more:
            send_edges(phase + 1, fields[k + depth], levels[0, 0])
        for step in range(depth):
            products = full_image(k + step, currents[step], recurrence[k + step], fields)
            row = row + line_up(products, at)
            at += len(products)
        k += depth
    send_row(1, row)
    gram = symmetric(take_row(1, at), ITERS + 1)
    upper, inverse = factor(gram)
    images = project(upper, inverse, [(a, g, b) for a, g, b, _ in recurrence])
    start, vectors, columns = arnoldi(upper, inverse, images, ITERS)
    weights = expand(least_squares(columns, start), vectors, upper, inverse)

    sol_p = add([w * f[0] for w, f in zip(weights, fields)])
    sol_v = add([w * f[1] for w, f in zip(weights, fields)])

    def gather(c, carry):
        at = c * CHUNK
        parts = [weights[i][None] * basis[i, pl.ds(at + 1, CHUNK)] for i in range(ITERS)]
        basis[ITERS, pl.ds(at + 1, CHUNK)] = add(parts)
        return carry

    lax.fori_loop(0, shells // CHUNK, gather, 0)
    flat = jnp.concatenate([basis[ITERS, 1 : shells + 1, s, :] for s in range(subs)], axis=0)
    turned[...] = flat.T
    stores = []
    for x in range(cx):
        for g in range(groups):
            edge_row = g * cells + x * cy
            stores.append(
                pltpu.make_async_copy(
                    turned.at[edge_row : edge_row + cy, :],
                    sol_conc_ref.at[x, :, g * span : (g + 1) * span],
                    out_sem.at[x, g],
                )
            )
    for copy in stores:
        copy.start()
    flat_p = jnp.concatenate(
        [sol_p[:, g * cells : (g + 1) * cells] for g in range(groups)] + [sol_v[:1, :cells]], axis=0
    )
    sol_pots_ref[...] = flat_p.T.reshape(cx, cy, nodes + 1)

    for phase in range(len(PLAN)):
        for o, copy in copies_of(phase):
            pl.when(there[o])(copy.wait_send)
    for o, copy, _ in fixed_moves:
        pl.when(there[o])(copy.wait_send)
    for step in range(2):
        part = rows.at[step, pl.ds(0, count - 1)]
        pltpu.make_async_copy(part, part, row_send.at[step]).wait()
    for copy in stores:
        copy.wait()


def solution(mesh):
    sizes = (mesh.shape["gx"], mesh.shape["gy"])
    count = sizes[0] * sizes[1]

    def shards(rhs_conc, rhs_pots, diffusion, exchange, slope):
        cx, cy = rhs_conc.shape[0], rhs_conc.shape[1]
        cells = cx * cy
        nodes = exchange.shape[2]
        shells = rhs_conc.shape[2] // nodes
        groups = LANES // cells
        subs = nodes // groups
        deepest = max(PLAN)
        near = len(surroundings(cx, cy, deepest))
        phases = len(PLAN)
        vmem = pl.BlockSpec(memory_space=pltpu.VMEM)
        anywhere = pl.BlockSpec(memory_space=pl.ANY)
        dma = pltpu.SemaphoreType.DMA
        return pl.pallas_call(
            functools.partial(cycle, sizes),
            out_shape=(
                jax.ShapeDtypeStruct(rhs_conc.shape, jnp.float32),
                jax.ShapeDtypeStruct(rhs_pots.shape, jnp.float32),
            ),
            in_specs=[anywhere] * 5,
            out_specs=(anywhere, vmem),
            scratch_shapes=[
                pltpu.VMEM((LANES, subs * shells), jnp.float32),
                pltpu.VMEM((ITERS + 1, shells + 2, subs, LANES), jnp.float32),
                pltpu.VMEM(rhs_pots.shape, jnp.float32),
                pltpu.VMEM((3,) + exchange.shape, jnp.float32),
                pltpu.VMEM((phases, deepest + 1, subs, LANES), jnp.float32),
                pltpu.VMEM((phases, near, deepest + 1, subs, LANES), jnp.float32),
                pltpu.VMEM((3, subs, LANES), jnp.float32),
                pltpu.VMEM((near, 3, subs, LANES), jnp.float32),
                pltpu.VMEM((2, count, 1, LANES), jnp.float32),
                pltpu.VMEM((2, 1, LANES), jnp.float32),
                dma((phases, near)),
                dma((phases, near)),
                dma((near,)),
                dma((near,)),
                dma((2,)),
                dma((2,)),
                dma((cx, groups)),
                dma((4,)),
                dma((cx, groups)),
            ],
            compiler_params=pltpu.CompilerParams(collective_id=0, has_side_effects=True),
        )(rhs_conc, rhs_pots, diffusion, exchange, slope)

    spec = P("gx", "gy", None)
    return jax.shard_map(
        shards,
        mesh=mesh,
        in_specs=(spec,) * 5,
        out_specs=(spec, spec),
        check_vma=False,
    )
```

```python
import functools

import jax
import jax.numpy as jnp
from jax import lax
from jax.experimental import pallas as pl
from jax.experimental.pallas import tpu as pltpu
from jax.sharding import PartitionSpec as P

ITERS = 10
LANES = 128
CHUNK = 16
PLAN = (3, 4, 3)
ADAPTIVE = 2

node_cond = 1.0
plane_cond = 0.5
collector_cond = 2.0
epsilon = 1e-06
center = 10.0
radius = 10.0
least_height = 0.05
least_pivot = 3e-07
MESH = pl.DeviceIdType.MESH


def add(terms):
    terms = [t for t in terms if t is not None]
    while len(terms) > 1:
        pairs = [terms[k] + terms[k + 1] for k in range(0, len(terms) - 1, 2)]
        terms = pairs + ([terms[-1]] if len(terms) % 2 else [])
    return terms[0]


def factor(gram):
    size = len(gram)
    left = [[gram[i][j] for j in range(size)] for i in range(size)]
    upper = [[None] * size for _ in range(size)]
    inverse = []
    for k in range(size):
        pivot = left[k][k]
        good = pivot > least_pivot * gram[k][k]
        inv = jnp.where(good, lax.rsqrt(jnp.where(good, pivot, 1.0)), 0.0)
        inverse.append(inv)
        upper[k][k] = pivot * inv
        for j in range(k + 1, size):
            upper[k][j] = left[k][j] * inv
        for i in range(k + 1, size):
            for j in range(i, size):
                left[i][j] = left[i][j] - upper[k][i] * upper[k][j]
    return upper, inverse


def project(upper, inverse, recurrence):
    columns = []
    for k, (alpha, gamma, beta) in enumerate(recurrence):
        column = []
        for i in range(k + 2):
            terms = [beta * upper[i][k + 1]]
            if i <= k:
                terms.append(alpha * upper[i][k])
            if i <= k - 1 and gamma is not None:
                terms.append(gamma * upper[i][k - 1])
            value = add(terms)
            known = [columns[m][i] * upper[m][k] for m in range(max(i - 1, 0), k)]
            if known:
                value = value - add(known)
            column.append(value * inverse[k])
        columns.append(column)
    return columns


def arnoldi(upper, inverse, images, count):
    height = jnp.sqrt(upper[0][0] * upper[0][0] + epsilon)
    start = height
    vectors = [[upper[0][0] / height]]
    columns = []
    for j in range(count):
        newest = vectors[j]
        image = [
            add([images[k][t] * newest[k] for k in range(max(t - 1, 0), j + 1)])
            for t in range(j + 2)
        ]
        coeffs = [
            add([vectors[i][t] * image[t] for t in range(i + 1)]) for i in range(j + 1)
        ]
        rest = [
            image[t] - add([coeffs[i] * vectors[i][t] for i in range(t, j + 1)])
            for t in range(j + 1)
        ] + [image[j + 1]]
        height = jnp.sqrt(add([r * r for r in rest]) + epsilon)
        columns.append(coeffs + [height])
        if j + 1 < count:
            scale = 1.0 / height
            vectors.append([r * scale for r in rest])
    return start, vectors, columns


def least_squares(columns, start):
    target, cosines, sines, uppers = [start], [], [], []
    for step, column in enumerate(columns):
        entries = list(column)
        for row in range(step):
            first = cosines[row] * entries[row] + sines[row] * entries[row + 1]
            second = cosines[row] * entries[row + 1] - sines[row] * entries[row]
            entries[row] = first
            entries[row + 1] = second
        size = jnp.sqrt(entries[step] * entries[step] + entries[step + 1] * entries[step + 1])
        shrink = 1.0 / size
        cosine = entries[step] * shrink
        sine = entries[step + 1] * shrink
        entries[step] = size
        cosines.append(cosine)
        sines.append(sine)
        lead = target[step]
        target[step] = cosine * lead
        target.append(-sine * lead)
        uppers.append((entries[: step + 1], shrink))
    weights = [None] * len(columns)
    for row in range(len(columns) - 1, -1, -1):
        total = target[row]
        for later in range(len(columns) - 1, row, -1):
            total = total - uppers[later][0][row] * weights[later]
        weights[row] = total * uppers[row][1]
    return weights


def expand(weights, vectors, upper, inverse):
    count = len(weights)
    along = [add([vectors[j][t] * weights[j] for j in range(t, count)]) for t in range(count)]
    out = [None] * count
    for row in range(count - 1, -1, -1):
        total = along[row]
        for later in range(count - 1, row, -1):
            total = total - upper[row][later] * out[later]
        out[row] = total * inverse[row]
    return out


def surroundings(cx, cy, depth):
    def away(extent, offset):
        return (abs(offset) - 1) * extent + 1 if offset else 0

    found = {}
    for a in range(-depth, depth + 1):
        for b in range(-depth, depth + 1):
            distance = away(cx, a) + away(cy, b)
            if 0 < distance <= depth:
                found[a, b] = distance
    return found


def cycle(
    sizes,
    conc_ref,
    pots_ref,
    diff_ref,
    exch_ref,
    slope_ref,
    sol_turned_ref,
    sol_pots_ref,
    turned,
    basis,
    raw_pots,
    raw_fixed,
    sent,
    halos,
    fixed_sent,
    fixed_halos,
    rows,
    sent_rows,
    edge_send,
    edge_recv,
    fixed_send,
    fixed_recv,
    row_send,
    row_recv,
    load_sem,
    small_sem,
):
    nx, ny = sizes
    count = nx * ny
    cx, cy = conc_ref.shape[0], conc_ref.shape[1]
    cells = cx * cy
    nodes = exch_ref.shape[2]
    shells = conc_ref.shape[2] // nodes
    groups = LANES // cells
    subs = nodes // groups
    mx = lax.axis_index("gx")
    my = lax.axis_index("gy")
    me = mx * ny + my
    deepest = max(PLAN)
    around = surroundings(cx, cy, deepest)
    order = sorted(around, key=lambda o: -around[o])
    place = {o: i for i, o in enumerate(order)}

    def peers(act):
        if count <= 32:
            for dx in range(nx - 1, -1, -1):
                for dy in range(ny - 1, -1, -1):
                    if dx or dy:
                        act(lax.rem(mx + dx, nx), lax.rem(my + dy, ny))
        else:

            def one(p, carry):
                other = lax.rem(me + p, count)
                act(lax.div(other, ny), lax.rem(other, ny))
                return carry

            lax.fori_loop(1, count, one, 0)

    barrier = pltpu.get_barrier_semaphore()
    peers(
        lambda px, py: pl.semaphore_signal(
            barrier, inc=1, device_id={"gx": px, "gy": py}, device_id_type=MESH
        )
    )

    span = subs * shells
    loads = []
    for x in range(cx):
        for g in range(groups):
            edge_row = g * cells + x * cy
            loads.append(
                pltpu.make_async_copy(
                    conc_ref.at[x, :, g * span : (g + 1) * span],
                    turned.at[edge_row : edge_row + cy, :],
                    load_sem.at[x, g],
                )
            )
    small = [pltpu.make_async_copy(pots_ref, raw_pots, small_sem.at[0])]
    for k, ref in enumerate((exch_ref, slope_ref, diff_ref)):
        small.append(pltpu.make_async_copy(ref, raw_fixed.at[k], small_sem.at[k + 1]))
    for copy in small + loads:
        copy.start()
    for copy in small:
        copy.wait()

    def fold_nodes(block):
        return block.reshape(cells, block.shape[2]).T

    def node_register(flat_t):
        return jnp.concatenate(
            [flat_t[g * subs : (g + 1) * subs, :] for g in range(groups)], axis=1
        )

    exch = node_register(fold_nodes(raw_fixed[0]))
    slope = node_register(fold_nodes(raw_fixed[1]))
    diff = node_register(fold_nodes(raw_fixed[2]))
    pots_t = fold_nodes(raw_pots[...])
    pot = node_register(pots_t)
    vol_row = pots_t[nodes : nodes + 1, :]
    vol = jnp.broadcast_to(jnp.concatenate([vol_row] * groups, axis=1), (subs, LANES))
    for k, value in enumerate((exch, slope, diff)):
        fixed_sent[k] = value

    lane = lax.broadcasted_iota(jnp.int32, (subs, LANES), 1)
    sub = lax.broadcasted_iota(jnp.int32, (subs, LANES), 0)
    group = lane // cells
    cell = lane % cells
    cell_x = cell // cy
    cell_y = cell % cy
    single = ((sub == 0) & (group == 0)).astype(jnp.float32)
    first_sub, last_sub = sub == 0, sub == subs - 1
    first_group, last_group = group == 0, group == groups - 1
    low_x, high_x = cell_x == 0, cell_x == cx - 1
    low_y, high_y = cell_y == 0, cell_y == cy - 1
    zero = jnp.zeros((subs, LANES), jnp.float32)

    there = {}
    for a, b in order:
        there[a, b] = (
            (mx + a >= 0) & (mx + a < nx) & (my + b >= 0) & (my + b < ny)
        )

    def roll(value, shift, axis=1):
        shift = shift % value.shape[axis]
        return pltpu.roll(value, shift, axis) if shift else value

    def sides(p, low_block, high_block, edge_low, edge_high, step, wide):
        low = roll(p, step)
        low = jnp.where(edge_low, zero if low_block is None else roll(low_block, -wide), low)
        high = roll(p, -step)
        high = jnp.where(edge_high, zero if high_block is None else roll(high_block, wide), high)
        return low + high

    def plane(p, near, member):
        def at(offset):
            return None if near[offset] is None else near[offset][member]

        across = sides(p, at((-1, 0)), at((1, 0)), low_x, high_x, cy, (cx - 1) * cy)
        along = sides(p, at((0, -1)), at((0, 1)), low_y, high_y, 1, cy - 1)
        return 4.0 * p - (across + along)

    def node_mirror(p):
        low = roll(p, 1, 0)
        inner = jnp.where(first_sub, jnp.where(first_group, p, roll(low, cells)), low)
        high = roll(p, -1, 0)
        outer = jnp.where(last_sub, jnp.where(last_group, p, roll(high, -cells)), high)
        return 2.0 * p - inner - outer

    def node_mean(value):
        total = jnp.broadcast_to(jnp.sum(value, axis=0, keepdims=True), (subs, LANES))
        parts = [total] + [roll(total, g * cells) for g in range(1, groups)]
        return add(parts) * (1.0 / nodes)

    nowhere = {(-1, 0): None, (1, 0): None, (0, -1): None, (0, 1): None}

    def pots_image(field, near, surface, fixed):
        p, v = field
        current = fixed[0] * (p - v)
        new_p = (
            node_cond * node_mirror(p)
            + current
            - fixed[1] * surface
            + plane_cond * plane(p, near, 0)
        )
        new_v = collector_cond * plane(v, near, 1) - node_mean(current)
        return new_p, new_v, current

    def relate(image, here, before, terms):
        alpha, gamma, _, inverse = terms
        value = image - alpha * here
        if gamma is not None:
            value = value - gamma * before
        return value * inverse

    def shell_images(levels, before, current, diffusion, terms):
        out = []
        for k in range(len(levels) - 1):
            here = levels[k]
            image = here + diffusion * (
                here - levels[k + 1] if k == 0 else 2.0 * here - levels[k - 1] - levels[k + 1]
            )
            if k == 0:
                image = image + current
            out.append(relate(image, here, before[k] if before else None, terms))
        return out

    def full_image(k, current, terms, fields, source=None, target=None):
        alpha, gamma, _, inverse = terms
        keep = (1.0 - alpha) * inverse
        spread = diff * inverse
        middle = (keep + 2.0 * spread)[None]
        spread = spread[None]
        basis[k, 0] = basis[k, 1]
        basis[k, shells + 1] = basis[k, shells]
        newest = fields[k + 1]
        starts = [
            fields[i][0] * newest[0] + fields[i][1] * (newest[1] * single) for i in range(k + 2)
        ]
        pushed = inverse * current

        def part(at, carry, last):
            here = basis[k, pl.ds(at + 1, CHUNK)]
            low = basis[k, pl.ds(at, CHUNK)]
            high = basis[k, pl.ds(at + 2, CHUNK)]
            new = middle * here - spread * (low + high)
            if gamma is not None:
                new = new - (gamma * inverse) * basis[k - 1, pl.ds(at + 1, CHUNK)]
            if last:
                new = jnp.concatenate([new[:-1], new[-1:] + pushed[None]], axis=0)
            basis[k + 1, pl.ds(at + 1, CHUNK)] = new
            others = [basis[i, pl.ds(at + 1, CHUNK)] for i in range(k)] + [here, new]
            return tuple(c + jnp.sum(o * new, axis=0) for c, o in zip(carry, others))

        parts = shells // CHUNK
        carry = lax.fori_loop(
            0, parts - 1, lambda c, carry: part(c * CHUNK, carry, False), tuple(starts)
        )
        return list(part((parts - 1) * CHUNK, carry, True))

    def line_up(products, offset):
        padded = -(-len(products) // 8) * 8
        stacked = [jnp.sum(d, axis=0, keepdims=True) for d in products]
        stacked += [zero[:1]] * (padded - len(products))
        tall = jnp.sum(jnp.concatenate(stacked, axis=0), axis=1, keepdims=True)
        at_row = lax.broadcasted_iota(jnp.int32, (padded, LANES), 0) + offset
        at_lane = lax.broadcasted_iota(jnp.int32, (padded, LANES), 1)
        return jnp.sum(jnp.where(at_row == at_lane, tall, 0.0), axis=0, keepdims=True)

    def row_copy(step, px, py):
        return pltpu.make_async_remote_copy(
            src_ref=sent_rows.at[step],
            dst_ref=rows.at[step, me],
            send_sem=row_send.at[step],
            recv_sem=row_recv.at[step],
            device_id={"gx": px, "gy": py},
            device_id_type=MESH,
        )

    def send_row_only(step):
        peers(lambda px, py: row_copy(step, px, py).start())

    def send_row(step, row):
        sent_rows[step] = row
        rows[step, me] = row
        send_row_only(step)

    def take_row(step, wanted):
        part = rows.at[step, pl.ds(0, count - 1)]
        pltpu.make_async_copy(part, part, row_recv.at[step]).wait()
        total = jnp.sum(rows[step], axis=0)
        return [jnp.broadcast_to(total[:, k : k + 1], (subs, LANES)) for k in range(wanted)]

    def copies_of(phase):
        depth = PLAN[phase]
        out = []
        for o in order:
            if around[o] > depth:
                continue
            a, b = o
            items = 2 + depth - around[o]
            out.append(
                (
                    o,
                    pltpu.make_async_remote_copy(
                        src_ref=sent.at[phase, pl.ds(0, items)],
                        dst_ref=halos.at[phase, place[-a, -b], pl.ds(0, items)],
                        send_sem=edge_send.at[phase, place[o]],
                        recv_sem=edge_recv.at[phase, place[-a, -b]],
                        device_id={
                            "gx": lax.rem(mx + a + nx * deepest, nx),
                            "gy": lax.rem(my + b + ny * deepest, ny),
                        },
                        device_id_type=MESH,
                    ),
                )
            )
        return out

    def arrivals_of(phase):
        depth = PLAN[phase]
        out = []
        for o in order:
            if around[o] > depth:
                continue
            items = 2 + depth - around[o]
            part = halos.at[phase, place[o], pl.ds(0, items)]
            out.append((o, pltpu.make_async_copy(part, part, edge_recv.at[phase, place[o]])))
        return out

    def fixed_copies():
        out = []
        for o in order:
            if around[o] > deepest - 1:
                continue
            a, b = o
            items = 3 if around[o] <= deepest - 2 else 2
            part = fixed_halos.at[place[o], pl.ds(0, items)]
            out.append(
                (
                    o,
                    pltpu.make_async_remote_copy(
                        src_ref=fixed_sent.at[pl.ds(0, items)],
                        dst_ref=fixed_halos.at[place[-a, -b], pl.ds(0, items)],
                        send_sem=fixed_send.at[place[o]],
                        recv_sem=fixed_recv.at[place[-a, -b]],
                        device_id={
                            "gx": lax.rem(mx + a + nx * deepest, nx),
                            "gy": lax.rem(my + b + ny * deepest, ny),
                        },
                        device_id_type=MESH,
                    ),
                    pltpu.make_async_copy(part, part, fixed_recv.at[place[o]]),
                )
            )
        return out

    def start_edges(phase):
        for o, copy in copies_of(phase):
            pl.when(there[o])(copy.start)

    def send_edges(phase, field, levels):
        sent[phase, 0] = field[0]
        sent[phase, 1] = field[1]
        for k, level in enumerate(levels):
            sent[phase, 2 + k] = level
        start_edges(phase)

    def tops(k, number):
        return [basis[k, shells - j] for j in range(number)]

    for copy in loads:
        copy.wait()
    turned_t = turned[...].T.reshape(subs, shells, LANES)
    for s in range(subs):
        basis[0, 1 : shells + 1, s, :] = turned_t[s]

    fields = [(pot, vol)] + [None] * ITERS
    fixed_own = (exch, slope)
    guess = [(center, None, radius, 1.0 / radius), (center, radius / 2, radius / 2, 2.0 / radius)]

    local = [fields[0]]
    products = [
        pot * pot
        + vol * (vol * single)
        + lax.fori_loop(
            0,
            shells // CHUNK,
            lambda c, t: t
            + jnp.sum(
                basis[0, pl.ds(c * CHUNK + 1, CHUNK)] * basis[0, pl.ds(c * CHUNK + 1, CHUNK)],
                axis=0,
            ),
            zero,
        )
    ]
    first_square = products[0]
    for k in range(ADAPTIVE):
        new_p, new_v, current = pots_image(local[k], nowhere, basis[k, shells], fixed_own)
        before = local[k - 1] if k else (None, None)
        local.append(
            (
                relate(new_p, local[k][0], before[0], guess[k]),
                relate(new_v, local[k][1], before[1], guess[k]),
            )
        )
        products += full_image(k, current, guess[k], local)
    local_row = line_up(products, 0)
    sent[0, 0] = pot
    sent[0, 1] = vol
    for i, level in enumerate(tops(0, PLAN[0] - 1)):
        sent[0, 2 + i] = level
    sent_rows[0] = local_row
    rows[0, me] = local_row
    pl.semaphore_wait(barrier, count - 1)
    send_row_only(0)
    start_edges(0)
    fixed_moves = fixed_copies()
    for o, copy, _ in fixed_moves:
        pl.when(there[o])(copy.start)

    def symmetric(sums, size):
        gram = [[None] * size for _ in range(size)]
        at = 0
        for j in range(size):
            for i in range(j + 1):
                gram[i][j] = gram[j][i] = sums[at]
                at += 1
        return gram

    def lanczos(sums):
        upper, inverse = factor(symmetric(sums, ADAPTIVE + 1))
        columns = project(upper, inverse, [(a, g, b) for a, g, b, _ in guess])
        out = []
        for k in range(ADAPTIVE):
            height = jnp.maximum(columns[k][k + 1], least_height)
            gamma = columns[k][k - 1] if k else None
            out.append((columns[k][k], gamma, height, 1.0 / height))
        return out

    recurrence = None
    row = line_up([first_square], 0)
    at = 1
    k = 0
    earlier = {}
    for phase, depth in enumerate(PLAN):
        more = phase + 1 < len(PLAN)
        ahead = PLAN[phase + 1] - 1 if more else 0
        if phase == 0:
            recurrence = lanczos(take_row(0, len(products)))
        for step in range(depth):
            if k + step < ADAPTIVE:
                continue
            gamma = radius / 2 if step or depth <= 2 else None
            beta = radius if gamma is None else radius / 2
            recurrence.append((center, gamma, beta, 1.0 / beta))
        for o, copy in arrivals_of(phase):
            pl.when(there[o])(copy.wait)
        if phase == 0:
            fixed = {(0, 0): (exch, slope, diff)}
            for o, _, wait in fixed_moves:
                pl.when(there[o])(wait.wait)
            for o, _, _ in fixed_moves:
                fixed[o] = tuple(
                    jnp.where(there[o], fixed_halos[place[o], i], 0.0)
                    for i in range(3 if around[o] <= deepest - 2 else 2)
                )
        now = {(0, 0): fields[k]}
        levels = {(0, 0): tops(k, depth + ahead)}
        before = {(0, 0): tops(k - 1, depth + ahead - 1) if k else None}
        for o in order:
            if around[o] <= depth:
                now[o] = tuple(
                    jnp.where(there[o], halos[phase, place[o], i], 0.0) for i in range(2)
                )
                levels[o] = [
                    jnp.where(there[o], halos[phase, place[o], 2 + i], 0.0)
                    for i in range(depth - around[o])
                ]
                before[o] = None
        currents = []
        past = earlier
        if k:
            past = dict(earlier)
            past[0, 0] = fields[k - 1]
        for step in range(depth):
            terms = recurrence[k + step]
            reach = depth - step - 1
            new, new_levels = {}, {}
            for o in now:
                if o != (0, 0) and around[o] > reach:
                    continue
                near = {
                    side: now.get((o[0] + side[0], o[1] + side[1])) for side in nowhere
                }
                new_p, new_v, current = pots_image(now[o], near, levels[o][0], fixed[o])
                last = past.get(o, (None, None))
                p = relate(new_p, now[o][0], last[0], terms)
                v = relate(new_v, now[o][1], last[1], terms)
                if o != (0, 0):
                    p = jnp.where(there[o], p, 0.0)
                    v = jnp.where(there[o], v, 0.0)
                else:
                    currents.append(current)
                new[o] = (p, v)
                if len(levels[o]) > 1:
                    new_levels[o] = shell_images(
                        levels[o], before[o], current, fixed[o][2], terms
                    )
                else:
                    new_levels[o] = []
            past, now = now, new
            before, levels = levels, new_levels
            fields[k + step + 1] = now[0, 0]
        earlier = {o: f for o, f in past.items() if o != (0, 0)}
        if more:
            send_edges(phase + 1, fields[k + depth], levels[0, 0])
        for step in range(depth):
            products = full_image(k + step, currents[step], recurrence[k + step], fields)
            row = row + line_up(products, at)
            at += len(products)
        k += depth
    send_row(1, row)
    gram = symmetric(take_row(1, at), ITERS + 1)
    upper, inverse = factor(gram)
    images = project(upper, inverse, [(a, g, b) for a, g, b, _ in recurrence])
    start, vectors, columns = arnoldi(upper, inverse, images, ITERS)
    weights = expand(least_squares(columns, start), vectors, upper, inverse)

    sol_p = add([w * f[0] for w, f in zip(weights, fields)])
    sol_v = add([w * f[1] for w, f in zip(weights, fields)])

    def gather(c, carry):
        at = c * CHUNK
        parts = [weights[i][None] * basis[i, pl.ds(at + 1, CHUNK)] for i in range(ITERS)]
        basis[ITERS, pl.ds(at + 1, CHUNK)] = add(parts)
        return carry

    lax.fori_loop(0, shells // CHUNK, gather, 0)
    flat = jnp.concatenate([basis[ITERS, 1 : shells + 1, s, :] for s in range(subs)], axis=0)
    sol_turned_ref[...] = flat.T
    flat_p = jnp.concatenate(
        [sol_p[:, g * cells : (g + 1) * cells] for g in range(groups)] + [sol_v[:1, :cells]], axis=0
    )
    sol_pots_ref[...] = flat_p.T.reshape(cx, cy, nodes + 1)

    for phase in range(len(PLAN)):
        for o, copy in copies_of(phase):
            pl.when(there[o])(copy.wait_send)
    for o, copy, _ in fixed_moves:
        pl.when(there[o])(copy.wait_send)
    for step in range(2):
        part = rows.at[step, pl.ds(0, count - 1)]
        pltpu.make_async_copy(part, part, row_send.at[step]).wait()


def place_outputs(flat_ref, pots_ref, sol_conc_ref, sol_pots_ref, conc_sem, pots_sem):
    cx, cy = sol_conc_ref.shape[0], sol_conc_ref.shape[1]
    cells = cx * cy
    groups = LANES // cells
    span = flat_ref.shape[1]
    copies = [pltpu.make_async_copy(pots_ref, sol_pots_ref, pots_sem)]
    for x in range(cx):
        for g in range(groups):
            edge_row = g * cells + x * cy
            copies.append(
                pltpu.make_async_copy(
                    flat_ref.at[edge_row : edge_row + cy, :],
                    sol_conc_ref.at[x, :, g * span : (g + 1) * span],
                    conc_sem.at[x, g],
                )
            )
    for copy in copies:
        copy.start()
    for copy in copies:
        copy.wait()


def solution(mesh):
    sizes = (mesh.shape["gx"], mesh.shape["gy"])
    count = sizes[0] * sizes[1]

    def shards(rhs_conc, rhs_pots, diffusion, exchange, slope):
        cx, cy = rhs_conc.shape[0], rhs_conc.shape[1]
        cells = cx * cy
        nodes = exchange.shape[2]
        shells = rhs_conc.shape[2] // nodes
        groups = LANES // cells
        subs = nodes // groups
        deepest = max(PLAN)
        near = len(surroundings(cx, cy, deepest))
        phases = len(PLAN)
        vmem = pl.BlockSpec(memory_space=pltpu.VMEM)
        anywhere = pl.BlockSpec(memory_space=pl.ANY)
        dma = pltpu.SemaphoreType.DMA
        inputs = [
            pltpu.with_memory_space_constraint(x, pltpu.HBM)
            for x in (rhs_conc, rhs_pots, diffusion, exchange, slope)
        ]
        flat, sol_pots = pl.pallas_call(
            functools.partial(cycle, sizes),
            out_shape=(
                jax.ShapeDtypeStruct((LANES, subs * shells), jnp.float32),
                jax.ShapeDtypeStruct(rhs_pots.shape, jnp.float32),
            ),
            in_specs=[anywhere] * 5,
            out_specs=(vmem, vmem),
            scratch_shapes=[
                pltpu.VMEM((LANES, subs * shells), jnp.float32),
                pltpu.VMEM((ITERS + 1, shells + 2, subs, LANES), jnp.float32),
                pltpu.VMEM(rhs_pots.shape, jnp.float32),
                pltpu.VMEM((3,) + exchange.shape, jnp.float32),
                pltpu.VMEM((phases, deepest + 1, subs, LANES), jnp.float32),
                pltpu.VMEM((phases, near, deepest + 1, subs, LANES), jnp.float32),
                pltpu.VMEM((3, subs, LANES), jnp.float32),
                pltpu.VMEM((near, 3, subs, LANES), jnp.float32),
                pltpu.VMEM((2, count, 1, LANES), jnp.float32),
                pltpu.VMEM((2, 1, LANES), jnp.float32),
                dma((phases, near)),
                dma((phases, near)),
                dma((near,)),
                dma((near,)),
                dma((2,)),
                dma((2,)),
                dma((cx, groups)),
                dma((4,)),
            ],
            compiler_params=pltpu.CompilerParams(
                collective_id=0,
                has_side_effects=True,
                vmem_limit_bytes=12 * 1024 * 1024,
            ),
        )(*inputs)
        return pl.pallas_call(
            place_outputs,
            out_shape=(
                jax.ShapeDtypeStruct(rhs_conc.shape, jnp.float32),
                jax.ShapeDtypeStruct(rhs_pots.shape, jnp.float32),
            ),
            in_specs=[vmem, vmem],
            out_specs=(anywhere, anywhere),
            scratch_shapes=[dma((cx, groups)), dma],
            compiler_params=pltpu.CompilerParams(vmem_limit_bytes=12 * 1024 * 1024),
        )(flat, sol_pots)

    spec = P("gx", "gy", None)
    return jax.shard_map(
        shards,
        mesh=mesh,
        in_specs=(spec,) * 5,
        out_specs=(spec, spec),
        check_vma=False,
    )
```

```python
import functools

import jax
import jax.numpy as jnp
from jax import lax
from jax.experimental import pallas as pl
from jax.experimental.pallas import tpu as pltpu
from jax.sharding import PartitionSpec as P

ITERS = 10
LANES = 128
CHUNK = 16
PLAN = (5, 5)
ADAPTIVE = 2

node_cond = 1.0
plane_cond = 0.5
collector_cond = 2.0
epsilon = 1e-06
center = 10.0
radius = 10.0
least_height = 0.05
least_pivot = 3e-07
MESH = pl.DeviceIdType.MESH


def add(terms):
    terms = [t for t in terms if t is not None]
    while len(terms) > 1:
        pairs = [terms[k] + terms[k + 1] for k in range(0, len(terms) - 1, 2)]
        terms = pairs + ([terms[-1]] if len(terms) % 2 else [])
    return terms[0]


def factor(gram):
    size = len(gram)
    left = [[gram[i][j] for j in range(size)] for i in range(size)]
    upper = [[None] * size for _ in range(size)]
    inverse = []
    for k in range(size):
        pivot = left[k][k]
        good = pivot > least_pivot * gram[k][k]
        inv = jnp.where(good, lax.rsqrt(jnp.where(good, pivot, 1.0)), 0.0)
        inverse.append(inv)
        upper[k][k] = pivot * inv
        for j in range(k + 1, size):
            upper[k][j] = left[k][j] * inv
        for i in range(k + 1, size):
            for j in range(i, size):
                left[i][j] = left[i][j] - upper[k][i] * upper[k][j]
    return upper, inverse


def project(upper, inverse, recurrence):
    columns = []
    for k, (alpha, gamma, beta) in enumerate(recurrence):
        column = []
        for i in range(k + 2):
            terms = [beta * upper[i][k + 1]]
            if i <= k:
                terms.append(alpha * upper[i][k])
            if i <= k - 1 and gamma is not None:
                terms.append(gamma * upper[i][k - 1])
            value = add(terms)
            known = [columns[m][i] * upper[m][k] for m in range(max(i - 1, 0), k)]
            if known:
                value = value - add(known)
            column.append(value * inverse[k])
        columns.append(column)
    return columns


def arnoldi(upper, inverse, images, count):
    height = jnp.sqrt(upper[0][0] * upper[0][0] + epsilon)
    start = height
    vectors = [[upper[0][0] / height]]
    columns = []
    for j in range(count):
        newest = vectors[j]
        image = [
            add([images[k][t] * newest[k] for k in range(max(t - 1, 0), j + 1)])
            for t in range(j + 2)
        ]
        coeffs = [
            add([vectors[i][t] * image[t] for t in range(i + 1)]) for i in range(j + 1)
        ]
        rest = [
            image[t] - add([coeffs[i] * vectors[i][t] for i in range(t, j + 1)])
            for t in range(j + 1)
        ] + [image[j + 1]]
        height = jnp.sqrt(add([r * r for r in rest]) + epsilon)
        columns.append(coeffs + [height])
        if j + 1 < count:
            scale = 1.0 / height
            vectors.append([r * scale for r in rest])
    return start, vectors, columns


def least_squares(columns, start):
    target, cosines, sines, uppers = [start], [], [], []
    for step, column in enumerate(columns):
        entries = list(column)
        for row in range(step):
            first = cosines[row] * entries[row] + sines[row] * entries[row + 1]
            second = cosines[row] * entries[row + 1] - sines[row] * entries[row]
            entries[row] = first
            entries[row + 1] = second
        size = jnp.sqrt(entries[step] * entries[step] + entries[step + 1] * entries[step + 1])
        shrink = 1.0 / size
        cosine = entries[step] * shrink
        sine = entries[step + 1] * shrink
        entries[step] = size
        cosines.append(cosine)
        sines.append(sine)
        lead = target[step]
        target[step] = cosine * lead
        target.append(-sine * lead)
        uppers.append((entries[: step + 1], shrink))
    weights = [None] * len(columns)
    for row in range(len(columns) - 1, -1, -1):
        total = target[row]
        for later in range(len(columns) - 1, row, -1):
            total = total - uppers[later][0][row] * weights[later]
        weights[row] = total * uppers[row][1]
    return weights


def expand(weights, vectors, upper, inverse):
    count = len(weights)
    along = [add([vectors[j][t] * weights[j] for j in range(t, count)]) for t in range(count)]
    out = [None] * count
    for row in range(count - 1, -1, -1):
        total = along[row]
        for later in range(count - 1, row, -1):
            total = total - upper[row][later] * out[later]
        out[row] = total * inverse[row]
    return out


def surroundings(cx, cy, depth):
    def away(extent, offset):
        return (abs(offset) - 1) * extent + 1 if offset else 0

    found = {}
    for a in range(-depth, depth + 1):
        for b in range(-depth, depth + 1):
            distance = away(cx, a) + away(cy, b)
            if 0 < distance <= depth:
                found[a, b] = distance
    return found


def strip_slots(widths, room):
    out, page, at = [], 0, 0
    for width in widths:
        if at + width > room:
            page, at = page + 1, 0
        out.append((page, at, width))
        at += width
    return out


def phase_widths(depth):
    return [depth, depth] + list(range(depth - 1, 0, -1))


def pages_of(slots, number):
    return 1 + max(page for page, _, _ in slots[:number])


def cycle(
    sizes,
    conc_ref,
    pots_ref,
    diff_ref,
    exch_ref,
    slope_ref,
    sol_turned_ref,
    sol_pots_ref,
    turned,
    basis,
    raw_pots,
    raw_fixed,
    sent,
    strips,
    halos,
    fixed_sent,
    fixed_strips,
    fixed_halos,
    rows,
    sent_rows,
    edge_send,
    edge_recv,
    fixed_send,
    fixed_recv,
    row_send,
    row_recv,
    load_sem,
    small_sem,
):
    nx, ny = sizes
    count = nx * ny
    cx, cy = conc_ref.shape[0], conc_ref.shape[1]
    cells = cx * cy
    nodes = exch_ref.shape[2]
    shells = conc_ref.shape[2] // nodes
    groups = LANES // cells
    subs = nodes // groups
    mx = lax.axis_index("gx")
    my = lax.axis_index("gy")
    me = mx * ny + my
    deepest = max(PLAN)
    around = surroundings(cx, cy, deepest)
    order = sorted(around, key=lambda o: -around[o])
    place = {o: i for i, o in enumerate(order)}

    def peers(act):
        if count <= 32:
            for dx in range(nx - 1, -1, -1):
                for dy in range(ny - 1, -1, -1):
                    if dx or dy:
                        act(lax.rem(mx + dx, nx), lax.rem(my + dy, ny))
        else:

            def one(p, carry):
                other = lax.rem(me + p, count)
                act(lax.div(other, ny), lax.rem(other, ny))
                return carry

            lax.fori_loop(1, count, one, 0)

    barrier = pltpu.get_barrier_semaphore()
    peers(
        lambda px, py: pl.semaphore_signal(
            barrier, inc=1, device_id={"gx": px, "gy": py}, device_id_type=MESH
        )
    )

    span = subs * shells
    loads = []
    for x in range(cx):
        for g in range(groups):
            edge_row = g * cells + x * cy
            loads.append(
                pltpu.make_async_copy(
                    conc_ref.at[x, :, g * span : (g + 1) * span],
                    turned.at[edge_row : edge_row + cy, :],
                    load_sem.at[x, g],
                )
            )
    small = [pltpu.make_async_copy(pots_ref, raw_pots, small_sem.at[0])]
    for k, ref in enumerate((exch_ref, slope_ref, diff_ref)):
        small.append(pltpu.make_async_copy(ref, raw_fixed.at[k], small_sem.at[k + 1]))
    for copy in small + loads:
        copy.start()
    for copy in small:
        copy.wait()

    def fold_nodes(block):
        return block.reshape(cells, block.shape[2]).T

    def node_register(flat_t):
        return jnp.concatenate(
            [flat_t[g * subs : (g + 1) * subs, :] for g in range(groups)], axis=1
        )

    exch = node_register(fold_nodes(raw_fixed[0]))
    slope = node_register(fold_nodes(raw_fixed[1]))
    diff = node_register(fold_nodes(raw_fixed[2]))
    pots_t = fold_nodes(raw_pots[...])
    pot = node_register(pots_t)
    vol_row = pots_t[nodes : nodes + 1, :]
    vol = jnp.broadcast_to(jnp.concatenate([vol_row] * groups, axis=1), (subs, LANES))

    lane = lax.broadcasted_iota(jnp.int32, (subs, LANES), 1)
    sub = lax.broadcasted_iota(jnp.int32, (subs, LANES), 0)
    group = lane // cells
    cell = lane % cells
    cell_x = cell // cy
    cell_y = cell % cy
    single = ((sub == 0) & (group == 0)).astype(jnp.float32)
    first_sub, last_sub = sub == 0, sub == subs - 1
    first_group, last_group = group == 0, group == groups - 1
    low_x, high_x = cell_x == 0, cell_x == cx - 1
    low_y, high_y = cell_y == 0, cell_y == cy - 1
    zero = jnp.zeros((subs, LANES), jnp.float32)

    there = {}
    for a, b in order:
        there[a, b] = (
            (mx + a >= 0) & (mx + a < nx) & (my + b >= 0) & (my + b < ny)
        )

    def roll(value, shift, axis=1):
        shift = shift % value.shape[axis]
        return pltpu.roll(value, shift, axis) if shift else value

    def pack(values, slots, to_low):
        packed = [zero] * pages_of(slots, len(slots))
        for value, (page, at, width) in zip(values, slots):
            if to_low:
                held = (cell_y >= at) & (cell_y < at + width)
                packed[page] = jnp.where(held, roll(value, at), packed[page])
            else:
                held = (cell_y >= cy - at - width) & (cell_y < cy - at)
                packed[page] = jnp.where(held, roll(value, -at), packed[page])
        return packed

    def unpack(pages, slot, from_high):
        page, at, width = slot
        packed = pages[page]
        if from_high:
            return jnp.where(cell_y < width, roll(packed, -at), zero)
        return jnp.where(cell_y >= cy - width, roll(packed, at), zero)

    def phase_slots(phase):
        return strip_slots(phase_widths(PLAN[phase]), cy)

    fixed_slots = strip_slots([deepest - 1, deepest - 1, max(deepest - 2, 0)], cy)

    def items_of(phase, o):
        number = 2 + PLAN[phase] - around[o]
        return pages_of(phase_slots(phase), number) if o[1] else number

    def fixed_items_of(o):
        number = 3 if around[o] <= deepest - 2 else 2
        return pages_of(fixed_slots, number) if o[1] else number

    def sides(p, low_block, high_block, edge_low, edge_high, step, wide):
        low = roll(p, step)
        low = jnp.where(edge_low, zero if low_block is None else roll(low_block, -wide), low)
        high = roll(p, -step)
        high = jnp.where(edge_high, zero if high_block is None else roll(high_block, wide), high)
        return low + high

    def plane(p, near, member):
        def at(offset):
            return None if near[offset] is None else near[offset][member]

        across = sides(p, at((-1, 0)), at((1, 0)), low_x, high_x, cy, (cx - 1) * cy)
        along = sides(p, at((0, -1)), at((0, 1)), low_y, high_y, 1, cy - 1)
        return 4.0 * p - (across + along)

    def node_mirror(p):
        low = roll(p, 1, 0)
        inner = jnp.where(first_sub, jnp.where(first_group, p, roll(low, cells)), low)
        high = roll(p, -1, 0)
        outer = jnp.where(last_sub, jnp.where(last_group, p, roll(high, -cells)), high)
        return 2.0 * p - inner - outer

    def node_mean(value):
        total = jnp.broadcast_to(jnp.sum(value, axis=0, keepdims=True), (subs, LANES))
        parts = [total] + [roll(total, g * cells) for g in range(1, groups)]
        return add(parts) * (1.0 / nodes)

    nowhere = {(-1, 0): None, (1, 0): None, (0, -1): None, (0, 1): None}

    def pots_image(field, near, surface, fixed):
        p, v = field
        current = fixed[0] * (p - v)
        new_p = (
            node_cond * node_mirror(p)
            + current
            - fixed[1] * surface
            + plane_cond * plane(p, near, 0)
        )
        new_v = collector_cond * plane(v, near, 1) - node_mean(current)
        return new_p, new_v, current

    def relate(image, here, before, terms):
        alpha, gamma, _, inverse = terms
        value = image - alpha * here
        if gamma is not None:
            value = value - gamma * before
        return value * inverse

    def shell_images(levels, before, current, diffusion, terms):
        out = []
        for k in range(len(levels) - 1):
            here = levels[k]
            image = here + diffusion * (
                here - levels[k + 1] if k == 0 else 2.0 * here - levels[k - 1] - levels[k + 1]
            )
            if k == 0:
                image = image + current
            out.append(relate(image, here, before[k] if before else None, terms))
        return out

    def full_image(k, current, terms, fields, source=None, target=None):
        alpha, gamma, _, inverse = terms
        keep = (1.0 - alpha) * inverse
        spread = diff * inverse
        middle = (keep + 2.0 * spread)[None]
        spread = spread[None]
        basis[k, 0] = basis[k, 1]
        basis[k, shells + 1] = basis[k, shells]
        newest = fields[k + 1]
        starts = [
            fields[i][0] * newest[0] + fields[i][1] * (newest[1] * single) for i in range(k + 2)
        ]
        pushed = inverse * current

        def part(at, carry, last):
            here = basis[k, pl.ds(at + 1, CHUNK)]
            low = basis[k, pl.ds(at, CHUNK)]
            high = basis[k, pl.ds(at + 2, CHUNK)]
            new = middle * here - spread * (low + high)
            if gamma is not None:
                new = new - (gamma * inverse) * basis[k - 1, pl.ds(at + 1, CHUNK)]
            if last:
                new = jnp.concatenate([new[:-1], new[-1:] + pushed[None]], axis=0)
            basis[k + 1, pl.ds(at + 1, CHUNK)] = new
            others = [basis[i, pl.ds(at + 1, CHUNK)] for i in range(k)] + [here, new]
            return tuple(c + jnp.sum(o * new, axis=0) for c, o in zip(carry, others))

        parts = shells // CHUNK
        carry = lax.fori_loop(
            0, parts - 1, lambda c, carry: part(c * CHUNK, carry, False), tuple(starts)
        )
        return list(part((parts - 1) * CHUNK, carry, True))

    def line_up(products, offset):
        padded = -(-len(products) // 8) * 8
        stacked = [jnp.sum(d, axis=0, keepdims=True) for d in products]
        stacked += [zero[:1]] * (padded - len(products))
        tall = jnp.sum(jnp.concatenate(stacked, axis=0), axis=1, keepdims=True)
        at_row = lax.broadcasted_iota(jnp.int32, (padded, LANES), 0) + offset
        at_lane = lax.broadcasted_iota(jnp.int32, (padded, LANES), 1)
        return jnp.sum(jnp.where(at_row == at_lane, tall, 0.0), axis=0, keepdims=True)

    def row_copy(step, px, py):
        return pltpu.make_async_remote_copy(
            src_ref=sent_rows.at[step],
            dst_ref=rows.at[step, me],
            send_sem=row_send.at[step],
            recv_sem=row_recv.at[step],
            device_id={"gx": px, "gy": py},
            device_id_type=MESH,
        )

    def send_row_only(step):
        peers(lambda px, py: row_copy(step, px, py).start())

    def send_row(step, row):
        sent_rows[step] = row
        rows[step, me] = row
        send_row_only(step)

    def take_row(step, wanted):
        part = rows.at[step, pl.ds(0, count - 1)]
        pltpu.make_async_copy(part, part, row_recv.at[step]).wait()
        total = jnp.sum(rows[step], axis=0)
        return [jnp.broadcast_to(total[:, k : k + 1], (subs, LANES)) for k in range(wanted)]

    def copies_of(phase):
        depth = PLAN[phase]
        out = []
        for o in order:
            if around[o] > depth:
                continue
            a, b = o
            items = items_of(phase, o)
            out.append(
                (
                    o,
                    pltpu.make_async_remote_copy(
                        src_ref=strips.at[phase, (b + 1) // 2, pl.ds(0, items)]
                        if b
                        else sent.at[phase, pl.ds(0, items)],
                        dst_ref=halos.at[phase, place[-a, -b], pl.ds(0, items)],
                        send_sem=edge_send.at[phase, place[o]],
                        recv_sem=edge_recv.at[phase, place[-a, -b]],
                        device_id={
                            "gx": lax.rem(mx + a + nx * deepest, nx),
                            "gy": lax.rem(my + b + ny * deepest, ny),
                        },
                        device_id_type=MESH,
                    ),
                )
            )
        return out

    def arrivals_of(phase):
        depth = PLAN[phase]
        out = []
        for o in order:
            if around[o] > depth:
                continue
            items = items_of(phase, o)
            part = halos.at[phase, place[o], pl.ds(0, items)]
            out.append((o, pltpu.make_async_copy(part, part, edge_recv.at[phase, place[o]])))
        return out

    def fixed_copies():
        out = []
        for o in order:
            if around[o] > deepest - 1:
                continue
            a, b = o
            items = fixed_items_of(o)
            part = fixed_halos.at[place[o], pl.ds(0, items)]
            out.append(
                (
                    o,
                    pltpu.make_async_remote_copy(
                        src_ref=fixed_strips.at[(b + 1) // 2, pl.ds(0, items)]
                        if b
                        else fixed_sent.at[pl.ds(0, items)],
                        dst_ref=fixed_halos.at[place[-a, -b], pl.ds(0, items)],
                        send_sem=fixed_send.at[place[o]],
                        recv_sem=fixed_recv.at[place[-a, -b]],
                        device_id={
                            "gx": lax.rem(mx + a + nx * deepest, nx),
                            "gy": lax.rem(my + b + ny * deepest, ny),
                        },
                        device_id_type=MESH,
                    ),
                    pltpu.make_async_copy(part, part, fixed_recv.at[place[o]]),
                )
            )
        return out

    def start_edges(phase):
        for o, copy in copies_of(phase):
            pl.when(there[o])(copy.start)

    def store_edges(phase, field, levels):
        values = [field[0], field[1]] + list(levels)
        for k, value in enumerate(values):
            sent[phase, k] = value
        for k in range(2):
            for page, packed in enumerate(pack(values, phase_slots(phase), k == 0)):
                strips[phase, k, page] = packed

    def send_edges(phase, field, levels):
        store_edges(phase, field, levels)
        start_edges(phase)

    def tops(k, number):
        return [basis[k, shells - j] for j in range(number)]

    for copy in loads:
        copy.wait()
    turned_t = turned[...].T.reshape(subs, shells, LANES)
    for s in range(subs):
        basis[0, 1 : shells + 1, s, :] = turned_t[s]

    fields = [(pot, vol)] + [None] * ITERS
    fixed_own = (exch, slope)
    guess = [(center, None, radius, 1.0 / radius), (center, radius / 2, radius / 2, 2.0 / radius)]

    local = [fields[0]]
    products = [
        pot * pot
        + vol * (vol * single)
        + lax.fori_loop(
            0,
            shells // CHUNK,
            lambda c, t: t
            + jnp.sum(
                basis[0, pl.ds(c * CHUNK + 1, CHUNK)] * basis[0, pl.ds(c * CHUNK + 1, CHUNK)],
                axis=0,
            ),
            zero,
        )
    ]
    first_square = products[0]
    for k in range(ADAPTIVE):
        new_p, new_v, current = pots_image(local[k], nowhere, basis[k, shells], fixed_own)
        before = local[k - 1] if k else (None, None)
        local.append(
            (
                relate(new_p, local[k][0], before[0], guess[k]),
                relate(new_v, local[k][1], before[1], guess[k]),
            )
        )
        products += full_image(k, current, guess[k], local)
    local_row = line_up(products, 0)
    store_edges(0, fields[0], tops(0, PLAN[0] - 1))
    for k, value in enumerate((exch, slope, diff)):
        fixed_sent[k] = value
    for k in range(2):
        for page, packed in enumerate(pack((exch, slope, diff), fixed_slots, k == 0)):
            fixed_strips[k, page] = packed
    sent_rows[0] = local_row
    rows[0, me] = local_row
    pl.semaphore_wait(barrier, count - 1)
    send_row_only(0)
    start_edges(0)
    fixed_moves = fixed_copies()
    for o, copy, _ in fixed_moves:
        pl.when(there[o])(copy.start)

    def symmetric(sums, size):
        gram = [[None] * size for _ in range(size)]
        at = 0
        for j in range(size):
            for i in range(j + 1):
                gram[i][j] = gram[j][i] = sums[at]
                at += 1
        return gram

    def lanczos(sums):
        upper, inverse = factor(symmetric(sums, ADAPTIVE + 1))
        columns = project(upper, inverse, [(a, g, b) for a, g, b, _ in guess])
        out = []
        for k in range(ADAPTIVE):
            height = jnp.maximum(columns[k][k + 1], least_height)
            gamma = columns[k][k - 1] if k else None
            out.append((columns[k][k], gamma, height, 1.0 / height))
        return out

    recurrence = None
    row = line_up([first_square], 0)
    at = 1
    k = 0
    earlier = {}
    for phase, depth in enumerate(PLAN):
        more = phase + 1 < len(PLAN)
        ahead = PLAN[phase + 1] - 1 if more else 0
        if phase == 0:
            recurrence = lanczos(take_row(0, len(products)))
        for step in range(depth):
            if k + step < ADAPTIVE:
                continue
            gamma = radius / 2 if step or depth <= 2 else None
            beta = radius if gamma is None else radius / 2
            recurrence.append((center, gamma, beta, 1.0 / beta))
        for o, copy in arrivals_of(phase):
            pl.when(there[o])(copy.wait)
        if phase == 0:
            fixed = {(0, 0): (exch, slope, diff)}
            for o, _, wait in fixed_moves:
                pl.when(there[o])(wait.wait)
            for o, _, _ in fixed_moves:
                number = 3 if around[o] <= deepest - 2 else 2
                got = [
                    jnp.where(there[o], fixed_halos[place[o], i], 0.0)
                    for i in range(fixed_items_of(o))
                ]
                if o[1]:
                    got = [unpack(got, fixed_slots[i], o[1] > 0) for i in range(number)]
                fixed[o] = tuple(got)
        now = {(0, 0): fields[k]}
        levels = {(0, 0): tops(k, depth + ahead)}
        before = {(0, 0): tops(k - 1, depth + ahead - 1) if k else None}
        for o in order:
            if around[o] <= depth:
                number = 2 + depth - around[o]
                got = [
                    jnp.where(there[o], halos[phase, place[o], i], 0.0)
                    for i in range(items_of(phase, o))
                ]
                if o[1]:
                    slots = phase_slots(phase)
                    got = [unpack(got, slots[i], o[1] > 0) for i in range(number)]
                now[o] = tuple(got[:2])
                levels[o] = got[2:]
                before[o] = None
        currents = []
        past = earlier
        if k:
            past = dict(earlier)
            past[0, 0] = fields[k - 1]
        for step in range(depth):
            terms = recurrence[k + step]
            reach = depth - step - 1
            new, new_levels = {}, {}
            for o in now:
                if o != (0, 0) and around[o] > reach:
                    continue
                near = {
                    side: now.get((o[0] + side[0], o[1] + side[1])) for side in nowhere
                }
                new_p, new_v, current = pots_image(now[o], near, levels[o][0], fixed[o])
                last = past.get(o, (None, None))
                p = relate(new_p, now[o][0], last[0], terms)
                v = relate(new_v, now[o][1], last[1], terms)
                if o != (0, 0):
                    p = jnp.where(there[o], p, 0.0)
                    v = jnp.where(there[o], v, 0.0)
                else:
                    currents.append(current)
                new[o] = (p, v)
                if len(levels[o]) > 1:
                    new_levels[o] = shell_images(
                        levels[o], before[o], current, fixed[o][2], terms
                    )
                else:
                    new_levels[o] = []
            past, now = now, new
            before, levels = levels, new_levels
            fields[k + step + 1] = now[0, 0]
        earlier = {o: f for o, f in past.items() if o != (0, 0)}
        if more:
            send_edges(phase + 1, fields[k + depth], levels[0, 0])
        for step in range(depth):
            products = full_image(k + step, currents[step], recurrence[k + step], fields)
            row = row + line_up(products, at)
            at += len(products)
        k += depth
    send_row(1, row)
    gram = symmetric(take_row(1, at), ITERS + 1)
    upper, inverse = factor(gram)
    images = project(upper, inverse, [(a, g, b) for a, g, b, _ in recurrence])
    start, vectors, columns = arnoldi(upper, inverse, images, ITERS)
    weights = expand(least_squares(columns, start), vectors, upper, inverse)

    sol_p = add([w * f[0] for w, f in zip(weights, fields)])
    sol_v = add([w * f[1] for w, f in zip(weights, fields)])

    def gather(c, carry):
        at = c * CHUNK
        parts = [weights[i][None] * basis[i, pl.ds(at + 1, CHUNK)] for i in range(ITERS)]
        basis[ITERS, pl.ds(at + 1, CHUNK)] = add(parts)
        return carry

    lax.fori_loop(0, shells // CHUNK, gather, 0)
    flat = jnp.concatenate([basis[ITERS, 1 : shells + 1, s, :] for s in range(subs)], axis=0)
    sol_turned_ref[...] = flat.T
    flat_p = jnp.concatenate(
        [sol_p[:, g * cells : (g + 1) * cells] for g in range(groups)] + [sol_v[:1, :cells]], axis=0
    )
    sol_pots_ref[...] = flat_p.T.reshape(cx, cy, nodes + 1)

    for phase in range(len(PLAN)):
        for o, copy in copies_of(phase):
            pl.when(there[o])(copy.wait_send)
    for o, copy, _ in fixed_moves:
        pl.when(there[o])(copy.wait_send)
    for step in range(2):
        part = rows.at[step, pl.ds(0, count - 1)]
        pltpu.make_async_copy(part, part, row_send.at[step]).wait()


def place_outputs(flat_ref, pots_ref, sol_conc_ref, sol_pots_ref, conc_sem, pots_sem):
    cx, cy = sol_conc_ref.shape[0], sol_conc_ref.shape[1]
    cells = cx * cy
    groups = LANES // cells
    span = flat_ref.shape[1]
    copies = [pltpu.make_async_copy(pots_ref, sol_pots_ref, pots_sem)]
    for x in range(cx):
        for g in range(groups):
            edge_row = g * cells + x * cy
            copies.append(
                pltpu.make_async_copy(
                    flat_ref.at[edge_row : edge_row + cy, :],
                    sol_conc_ref.at[x, :, g * span : (g + 1) * span],
                    conc_sem.at[x, g],
                )
            )
    for copy in copies:
        copy.start()
    for copy in copies:
        copy.wait()


def solution(mesh):
    sizes = (mesh.shape["gx"], mesh.shape["gy"])
    count = sizes[0] * sizes[1]

    def shards(rhs_conc, rhs_pots, diffusion, exchange, slope):
        cx, cy = rhs_conc.shape[0], rhs_conc.shape[1]
        cells = cx * cy
        nodes = exchange.shape[2]
        shells = rhs_conc.shape[2] // nodes
        groups = LANES // cells
        subs = nodes // groups
        deepest = max(PLAN)
        near = len(surroundings(cx, cy, deepest))
        phases = len(PLAN)
        widest = strip_slots(phase_widths(deepest), cy)
        pages = pages_of(widest, len(widest))
        vmem = pl.BlockSpec(memory_space=pltpu.VMEM)
        anywhere = pl.BlockSpec(memory_space=pl.ANY)
        dma = pltpu.SemaphoreType.DMA
        inputs = [
            pltpu.with_memory_space_constraint(x, pltpu.HBM)
            for x in (rhs_conc, rhs_pots, diffusion, exchange, slope)
        ]
        flat, sol_pots = pl.pallas_call(
            functools.partial(cycle, sizes),
            out_shape=(
                jax.ShapeDtypeStruct((LANES, subs * shells), jnp.float32),
                jax.ShapeDtypeStruct(rhs_pots.shape, jnp.float32),
            ),
            in_specs=[anywhere] * 5,
            out_specs=(vmem, vmem),
            scratch_shapes=[
                pltpu.VMEM((LANES, subs * shells), jnp.float32),
                pltpu.VMEM((ITERS + 1, shells + 2, subs, LANES), jnp.float32),
                pltpu.VMEM(rhs_pots.shape, jnp.float32),
                pltpu.VMEM((3,) + exchange.shape, jnp.float32),
                pltpu.VMEM((phases, deepest + 1, subs, LANES), jnp.float32),
                pltpu.VMEM((phases, 2, pages, subs, LANES), jnp.float32),
                pltpu.VMEM((phases, near, deepest + 1, subs, LANES), jnp.float32),
                pltpu.VMEM((3, subs, LANES), jnp.float32),
                pltpu.VMEM((2, pages, subs, LANES), jnp.float32),
                pltpu.VMEM((near, 3, subs, LANES), jnp.float32),
                pltpu.VMEM((2, count, 1, LANES), jnp.float32),
                pltpu.VMEM((2, 1, LANES), jnp.float32),
                dma((phases, near)),
                dma((phases, near)),
                dma((near,)),
                dma((near,)),
                dma((2,)),
                dma((2,)),
                dma((cx, groups)),
                dma((4,)),
            ],
            compiler_params=pltpu.CompilerParams(
                collective_id=0,
                has_side_effects=True,
                vmem_limit_bytes=12 * 1024 * 1024,
            ),
        )(*inputs)
        return pl.pallas_call(
            place_outputs,
            out_shape=(
                jax.ShapeDtypeStruct(rhs_conc.shape, jnp.float32),
                jax.ShapeDtypeStruct(rhs_pots.shape, jnp.float32),
            ),
            in_specs=[vmem, vmem],
            out_specs=(anywhere, anywhere),
            scratch_shapes=[dma((cx, groups)), dma],
            compiler_params=pltpu.CompilerParams(vmem_limit_bytes=12 * 1024 * 1024),
        )(flat, sol_pots)

    spec = P("gx", "gy", None)
    return jax.shard_map(
        shards,
        mesh=mesh,
        in_specs=(spec,) * 5,
        out_specs=(spec, spec),
        check_vma=False,
    )
```

```python
import functools

import jax
import jax.numpy as jnp
from jax import lax
from jax.experimental import pallas as pl
from jax.experimental.pallas import tpu as pltpu
from jax.sharding import PartitionSpec as P

ITERS = 10
LANES = 128
CHUNK = 16
PLAN = (5, 5)
ADAPTIVE = 2

node_cond = 1.0
plane_cond = 0.5
collector_cond = 2.0
epsilon = 1e-06
center = 10.0
radius = 10.0
least_height = 0.05
least_pivot = 3e-07
MESH = pl.DeviceIdType.MESH


def add(terms):
    terms = [t for t in terms if t is not None]
    while len(terms) > 1:
        pairs = [terms[k] + terms[k + 1] for k in range(0, len(terms) - 1, 2)]
        terms = pairs + ([terms[-1]] if len(terms) % 2 else [])
    return terms[0]


def factor_column(gram, upper, inverse):
    j = len(inverse)
    column = []
    for i in range(j):
        value = gram[i][j]
        if i:
            value = value - add([upper[i][m] * column[m] for m in range(i)])
        column.append(value * inverse[i])
    pivot = gram[j][j]
    if j:
        pivot = pivot - add([c * c for c in column])
    good = pivot > least_pivot * gram[j][j]
    inv = jnp.where(good, lax.rsqrt(jnp.where(good, pivot, 1.0)), 0.0)
    upper.append(column + [pivot * inv])
    inverse.append(inv)


def project_column(upper, inverse, recurrence, columns):
    k = len(columns)
    alpha, gamma, beta = recurrence[k]
    column = []
    for i in range(k + 2):
        terms = [beta * upper[k + 1][i]]
        if i <= k:
            terms.append(alpha * upper[k][i])
        if i <= k - 1 and gamma is not None:
            terms.append(gamma * upper[k - 1][i])
        value = add(terms)
        known = [columns[m][i] * upper[k][m] for m in range(max(i - 1, 0), k)]
        if known:
            value = value - add(known)
        column.append(value * inverse[k])
    columns.append(column)


def arnoldi_column(images, vectors):
    j = len(vectors) - 1
    newest = vectors[j]
    image = [
        add([images[k][t] * newest[k] for k in range(max(t - 1, 0), j + 1)]) for t in range(j + 2)
    ]
    coeffs = [add([vectors[i][t] * image[t] for t in range(i + 1)]) for i in range(j + 1)]
    rest = [
        image[t] - add([coeffs[i] * vectors[i][t] for i in range(t, j + 1)]) for t in range(j + 1)
    ] + [image[j + 1]]
    square = add([r * r for r in rest]) + epsilon
    scale = lax.rsqrt(square)
    height = square * scale
    vectors.append([r * scale for r in rest])
    return coeffs + [height]


def rotate_column(entries, target, cosines, sines, uppers):
    step = len(uppers)
    entries = list(entries)
    for row in range(step):
        first = cosines[row] * entries[row] + sines[row] * entries[row + 1]
        second = cosines[row] * entries[row + 1] - sines[row] * entries[row]
        entries[row] = first
        entries[row + 1] = second
    square = entries[step] * entries[step] + entries[step + 1] * entries[step + 1]
    shrink = lax.rsqrt(square)
    size = square * shrink
    cosine = entries[step] * shrink
    sine = entries[step + 1] * shrink
    entries[step] = size
    cosines.append(cosine)
    sines.append(sine)
    lead = target[step]
    target[step] = cosine * lead
    target.append(-sine * lead)
    uppers.append((entries[: step + 1], shrink))


def back_substitute(target, uppers):
    count = len(uppers)
    weights = [None] * count
    for row in range(count - 1, -1, -1):
        total = target[row]
        for later in range(count - 1, row, -1):
            total = total - uppers[later][0][row] * weights[later]
        weights[row] = total * uppers[row][1]
    return weights


def expand(weights, vectors, upper, inverse):
    count = len(weights)
    along = [add([vectors[j][t] * weights[j] for j in range(t, count)]) for t in range(count)]
    out = [None] * count
    for row in range(count - 1, -1, -1):
        total = along[row]
        for later in range(count - 1, row, -1):
            total = total - upper[later][row] * out[later]
        out[row] = total * inverse[row]
    return out


def surroundings(cx, cy, depth):
    def away(extent, offset):
        return (abs(offset) - 1) * extent + 1 if offset else 0

    found = {}
    for a in range(-depth, depth + 1):
        for b in range(-depth, depth + 1):
            distance = away(cx, a) + away(cy, b)
            if 0 < distance <= depth:
                found[a, b] = distance
    return found


def strip_slots(widths, room):
    out, page, at = [], 0, 0
    for width in widths:
        if at + width > room:
            page, at = page + 1, 0
        out.append((page, at, width))
        at += width
    return out


def phase_widths(depth):
    return [depth, depth] + list(range(depth - 1, 0, -1))


def pages_of(slots, number):
    return 1 + max(page for page, _, _ in slots[:number])


def cycle(
    sizes,
    conc_ref,
    pots_ref,
    diff_ref,
    exch_ref,
    slope_ref,
    sol_turned_ref,
    sol_pots_ref,
    turned,
    basis,
    raw_pots,
    raw_fixed,
    sent,
    strips,
    halos,
    rows,
    sent_rows,
    edge_send,
    edge_recv,
    row_send,
    row_recv,
    load_sem,
    small_sem,
):
    nx, ny = sizes
    count = nx * ny
    cx, cy = conc_ref.shape[0], conc_ref.shape[1]
    cells = cx * cy
    nodes = exch_ref.shape[2]
    shells = conc_ref.shape[2] // nodes
    groups = LANES // cells
    subs = nodes // groups
    mx = lax.axis_index("gx")
    my = lax.axis_index("gy")
    me = mx * ny + my
    deepest = max(PLAN)
    around = surroundings(cx, cy, deepest)
    order = sorted(around, key=lambda o: -around[o])
    place = {o: i for i, o in enumerate(order)}

    def peers(act):
        if count <= 32:
            for dx in range(nx - 1, -1, -1):
                for dy in range(ny - 1, -1, -1):
                    if dx or dy:
                        act(lax.rem(mx + dx, nx), lax.rem(my + dy, ny))
        else:

            def one(p, carry):
                other = lax.rem(me + p, count)
                act(lax.div(other, ny), lax.rem(other, ny))
                return carry

            lax.fori_loop(1, count, one, 0)

    barrier = pltpu.get_barrier_semaphore()
    peers(
        lambda px, py: pl.semaphore_signal(
            barrier, inc=1, device_id={"gx": px, "gy": py}, device_id_type=MESH
        )
    )

    span = subs * shells
    loads = []
    for x in range(cx):
        for g in range(groups):
            edge_row = g * cells + x * cy
            loads.append(
                pltpu.make_async_copy(
                    conc_ref.at[x, :, g * span : (g + 1) * span],
                    turned.at[edge_row : edge_row + cy, :],
                    load_sem.at[x, g],
                )
            )
    small = [pltpu.make_async_copy(pots_ref, raw_pots, small_sem.at[0])]
    for k, ref in enumerate((exch_ref, slope_ref, diff_ref)):
        small.append(pltpu.make_async_copy(ref, raw_fixed.at[k], small_sem.at[k + 1]))
    for copy in small + loads:
        copy.start()
    for copy in small:
        copy.wait()

    def fold_nodes(block):
        return block.reshape(cells, block.shape[2]).T

    def node_register(flat_t):
        return jnp.concatenate(
            [flat_t[g * subs : (g + 1) * subs, :] for g in range(groups)], axis=1
        )

    exch = node_register(fold_nodes(raw_fixed[0]))
    slope = node_register(fold_nodes(raw_fixed[1]))
    diff = node_register(fold_nodes(raw_fixed[2]))
    pots_t = fold_nodes(raw_pots[...])
    pot = node_register(pots_t)
    vol_row = pots_t[nodes : nodes + 1, :]
    vol = jnp.broadcast_to(jnp.concatenate([vol_row] * groups, axis=1), (subs, LANES))

    lane = lax.broadcasted_iota(jnp.int32, (subs, LANES), 1)
    sub = lax.broadcasted_iota(jnp.int32, (subs, LANES), 0)
    group = lane // cells
    cell = lane % cells
    cell_x = cell // cy
    cell_y = cell % cy
    single = ((sub == 0) & (group == 0)).astype(jnp.float32)
    first_sub, last_sub = sub == 0, sub == subs - 1
    first_group, last_group = group == 0, group == groups - 1
    low_x, high_x = cell_x == 0, cell_x == cx - 1
    low_y, high_y = cell_y == 0, cell_y == cy - 1
    zero = jnp.zeros((subs, LANES), jnp.float32)
    middle = (subs - 1) // 2

    there = {}
    for a, b in order:
        there[a, b] = (
            (mx + a >= 0) & (mx + a < nx) & (my + b >= 0) & (my + b < ny)
        )

    def roll(value, shift, axis=1):
        shift = shift % value.shape[axis]
        return pltpu.roll(value, shift, axis) if shift else value

    def pack(values, slots, to_low):
        packed = [zero] * pages_of(slots, len(slots))
        for value, (page, at, width) in zip(values, slots):
            if to_low:
                held = (cell_y >= at) & (cell_y < at + width)
                packed[page] = jnp.where(held, roll(value, at), packed[page])
            else:
                held = (cell_y >= cy - at - width) & (cell_y < cy - at)
                packed[page] = jnp.where(held, roll(value, -at), packed[page])
        return packed

    def unpack(pages, slot, from_high):
        page, at, width = slot
        packed = pages[page]
        if from_high:
            return jnp.where(cell_y < width, roll(packed, -at), zero)
        return jnp.where(cell_y >= cy - width, roll(packed, at), zero)

    def phase_slots(phase):
        return strip_slots(phase_widths(PLAN[phase]), cy)

    fixed_slots = strip_slots([deepest - 1, deepest - 1, max(deepest - 2, 0)], cy)

    def items_of(phase, o):
        number = 2 + PLAN[phase] - around[o]
        return pages_of(phase_slots(phase), number) if o[1] else number

    def first_of(phase, o):
        if phase:
            return 0
        if o[1]:
            return 0 if around[o] < deepest else 1
        return {0: 3, 1: 1}.get(deepest - around[o], 0)

    def offset_of(phase, b):
        return 0 if phase else 1 if b else 3

    def sides(p, low_block, high_block, edge_low, edge_high, step, wide):
        low = roll(p, step)
        low = jnp.where(edge_low, zero if low_block is None else roll(low_block, -wide), low)
        high = roll(p, -step)
        high = jnp.where(edge_high, zero if high_block is None else roll(high_block, wide), high)
        return low + high

    def plane(p, near, member):
        def at(offset):
            return None if near[offset] is None else near[offset][member]

        across = sides(p, at((-1, 0)), at((1, 0)), low_x, high_x, cy, (cx - 1) * cy)
        along = sides(p, at((0, -1)), at((0, 1)), low_y, high_y, 1, cy - 1)
        return 4.0 * p - (across + along)

    def node_mirror(p):
        low = roll(p, 1, 0)
        inner = jnp.where(first_sub, jnp.where(first_group, p, roll(low, cells)), low)
        high = roll(p, -1, 0)
        outer = jnp.where(last_sub, jnp.where(last_group, p, roll(high, -cells)), high)
        return 2.0 * p - inner - outer

    def node_mean(value):
        total = jnp.broadcast_to(jnp.sum(value, axis=0, keepdims=True), (subs, LANES))
        parts = [total] + [roll(total, g * cells) for g in range(1, groups)]
        return add(parts) * (1.0 / nodes)

    nowhere = {(-1, 0): None, (1, 0): None, (0, -1): None, (0, 1): None}

    def pots_image(field, near, surface, fixed):
        p, v = field
        current = fixed[0] * (p - v)
        new_p = (
            node_cond * node_mirror(p)
            + current
            - fixed[1] * surface
            + plane_cond * plane(p, near, 0)
        )
        new_v = collector_cond * plane(v, near, 1) - node_mean(current)
        return new_p, new_v, current

    def relate(image, here, before, terms):
        alpha, gamma, _, inverse = terms
        value = image - alpha * here
        if gamma is not None:
            value = value - gamma * before
        return value * inverse

    def shell_images(levels, before, current, diffusion, terms):
        out = []
        for k in range(len(levels) - 1):
            here = levels[k]
            image = here + diffusion * (
                here - levels[k + 1] if k == 0 else 2.0 * here - levels[k - 1] - levels[k + 1]
            )
            if k == 0:
                image = image + current
            out.append(relate(image, here, before[k] if before else None, terms))
        return out

    def pots_products(k, fields):
        newest = fields[k + 1]
        return [
            fields[i][0] * newest[0] + fields[i][1] * (newest[1] * single) for i in range(k + 2)
        ]

    def image_shells(k, current, terms, straight=False):
        alpha, gamma, _, inverse = terms
        keep = (1.0 - alpha) * inverse
        spread = diff * inverse
        middle_part = (keep + 2.0 * spread)[None]
        spread = spread[None]
        basis[k, 0] = basis[k, 1]
        basis[k, shells + 1] = basis[k, shells]
        pushed = inverse * current
        drag = None if gamma is None else gamma * inverse

        def part(at, carry, last):
            here = basis[k, pl.ds(at + 1, CHUNK)]
            low = basis[k, pl.ds(at, CHUNK)]
            high = basis[k, pl.ds(at + 2, CHUNK)]
            new = middle_part * here - spread * (low + high)
            others = [basis[i, pl.ds(at + 1, CHUNK)] for i in range(k)] + [here]
            if drag is not None:
                behind = others[k - 1]
                new = new - (behind if isinstance(drag, float) and drag == 1.0 else drag * behind)
            if last:
                new = jnp.concatenate([new[:-1], new[-1:] + pushed[None]], axis=0)
            basis[k + 1, pl.ds(at + 1, CHUNK)] = new
            return tuple(
                c + jnp.sum(o * new, axis=0) for c, o in zip(carry, others + [new])
            )

        parts = shells // CHUNK
        if straight:
            carry = (zero,) * (k + 2)
            for c in range(parts - 1):
                carry = part(c * CHUNK, carry, False)
            return list(part((parts - 1) * CHUNK, carry, True))
        carry = lax.fori_loop(
            0,
            parts - 1,
            lambda c, carry: part(c * CHUNK, carry, False),
            (zero,) * (k + 2),
        )
        return list(part((parts - 1) * CHUNK, carry, True))

    def line_up(products, offset):
        padded = -(-len(products) // 8) * 8
        stacked = [jnp.sum(d, axis=0, keepdims=True) for d in products]
        stacked += [zero[:1]] * (padded - len(products))
        tall = jnp.sum(jnp.concatenate(stacked, axis=0), axis=1, keepdims=True)
        at_row = lax.broadcasted_iota(jnp.int32, (padded, LANES), 0) + offset
        at_lane = lax.broadcasted_iota(jnp.int32, (padded, LANES), 1)
        return jnp.sum(jnp.where(at_row == at_lane, tall, 0.0), axis=0, keepdims=True)

    def row_copy(step, px, py):
        return pltpu.make_async_remote_copy(
            src_ref=sent_rows.at[step],
            dst_ref=rows.at[step, me],
            send_sem=row_send.at[step],
            recv_sem=row_recv.at[step],
            device_id={"gx": px, "gy": py},
            device_id_type=MESH,
        )

    def send_row_only(step):
        peers(lambda px, py: row_copy(step, px, py).start())

    def send_row(step, row):
        sent_rows[step] = row
        rows[step, me] = row
        send_row_only(step)

    def take_row(step, wanted):
        part = rows.at[step, pl.ds(0, count - 1)]
        pltpu.make_async_copy(part, part, row_recv.at[step]).wait()
        total = jnp.sum(rows[step], axis=0)
        return [jnp.broadcast_to(total[:, k : k + 1], (subs, LANES)) for k in range(wanted)]

    def copies_of(phase):
        depth = PLAN[phase]
        out = []
        for o in order:
            if around[o] > depth:
                continue
            a, b = o
            start = first_of(phase, o)
            items = offset_of(phase, b) + items_of(phase, o) - start
            out.append(
                (
                    o,
                    pltpu.make_async_remote_copy(
                        src_ref=strips.at[phase, (b + 1) // 2, pl.ds(start, items)]
                        if b
                        else sent.at[phase, pl.ds(start, items)],
                        dst_ref=halos.at[phase, place[-a, -b], pl.ds(start, items)],
                        send_sem=edge_send.at[phase, place[o]],
                        recv_sem=edge_recv.at[phase, place[-a, -b]],
                        device_id={
                            "gx": lax.rem(mx + a + nx * deepest, nx),
                            "gy": lax.rem(my + b + ny * deepest, ny),
                        },
                        device_id_type=MESH,
                    ),
                )
            )
        return out

    def arrivals_of(phase):
        depth = PLAN[phase]
        out = []
        for o in order:
            if around[o] > depth:
                continue
            start = first_of(phase, o)
            items = offset_of(phase, o[1]) + items_of(phase, o) - start
            part = halos.at[phase, place[o], pl.ds(start, items)]
            out.append((o, pltpu.make_async_copy(part, part, edge_recv.at[phase, place[o]])))
        return out

    def start_edges(phase):
        for o, copy in copies_of(phase):
            pl.when(there[o])(copy.start)

    def store_edges(phase, field, levels):
        values = [field[0], field[1]] + list(levels)
        for k, value in enumerate(values):
            sent[phase, offset_of(phase, 0) + k] = value
        for k in range(2):
            for page, packed in enumerate(pack(values, phase_slots(phase), k == 0)):
                strips[phase, k, offset_of(phase, 1) + page] = packed

    def send_edges(phase, field, levels):
        store_edges(phase, field, levels)
        start_edges(phase)

    def tops(k, number):
        return [basis[k, shells - j] for j in range(number)]

    for copy in loads:
        copy.wait()
    turned_t = turned[...].T.reshape(subs, shells, LANES)
    for s in range(subs):
        basis[0, 1 : shells + 1, s, :] = turned_t[s]

    fields = [(pot, vol)] + [None] * ITERS
    fixed_own = (exch, slope)
    guess = [(center, None, radius, 1.0 / radius), (center, radius / 2, radius / 2, 2.0 / radius)]

    local = [fields[0]]
    products = [
        pot * pot
        + vol * (vol * single)
        + lax.fori_loop(
            0,
            shells // CHUNK,
            lambda c, t: t
            + jnp.sum(
                basis[0, pl.ds(c * CHUNK + 1, CHUNK)] * basis[0, pl.ds(c * CHUNK + 1, CHUNK)],
                axis=0,
            ),
            zero,
        )
    ]
    first_square = products[0]
    for k in range(ADAPTIVE):
        new_p, new_v, current = pots_image(local[k], nowhere, basis[k, shells], fixed_own)
        before = local[k - 1] if k else (None, None)
        local.append(
            (
                relate(new_p, local[k][0], before[0], guess[k]),
                relate(new_v, local[k][1], before[1], guess[k]),
            )
        )
        inner = image_shells(k, current, guess[k])
        products += [c + o for c, o in zip(inner, pots_products(k, local))]
    local_row = line_up(products, 0)
    local_count = len(products)
    store_edges(0, fields[0], tops(0, PLAN[0] - 1))
    for k, value in enumerate((diff, exch, slope)):
        sent[0, k] = value
    for k in range(2):
        strips[0, k, 0] = pack((exch, slope, diff), fixed_slots, k == 0)[0]
    sent_rows[0] = local_row
    rows[0, me] = local_row
    pl.semaphore_wait(barrier, count - 1)
    start_edges(0)
    send_row_only(0)

    def symmetric(sums, size):
        gram = [[None] * size for _ in range(size)]
        at = 0
        for j in range(size):
            for i in range(j + 1):
                gram[i][j] = gram[j][i] = sums[at]
                at += 1
        return gram

    def lanczos(sums):
        gram = symmetric(sums, ADAPTIVE + 1)
        upper, inverse, columns = [], [], []
        for k in range(ADAPTIVE + 1):
            factor_column(gram, upper, inverse)
            if k:
                project_column(upper, inverse, [g[:3] for g in guess], columns)
        out = []
        for k in range(ADAPTIVE):
            height = jnp.maximum(columns[k][k + 1], least_height)
            gamma = columns[k][k - 1] if k else None
            out.append((columns[k][k], gamma, height, 1.0 / height))
        return out

    recurrence = None
    restart = (center, None, radius, 1.0 / radius)
    usual = (center, radius / 2, radius / 2, 2.0 / radius)
    products = [first_square]
    imaged = set()
    early = []
    k = 0
    for phase, depth in enumerate(PLAN):
        more = phase + 1 < len(PLAN)
        ahead = PLAN[phase + 1] - 1 if more else 0
        if phase == 0:
            recurrence = lanczos(take_row(0, local_count))
        for step in range(depth):
            if k + step < ADAPTIVE:
                continue
            recurrence.append(usual if step else restart)
        for o, copy in arrivals_of(phase):
            pl.when(there[o])(copy.wait)
        slots = phase_slots(phase)

        def taken(o):
            return [
                jnp.where(there[o], halos[phase, place[o], offset_of(phase, o[1]) + i], 0.0)
                for i in range(items_of(phase, o))
            ]

        def beside(got, page_slots, number):
            return [
                add([unpack(got[b], page_slots[i], b > 0) for b in got]) for i in range(number)
            ]

        pots = {(0, 0): fields[k][0]}
        levels = {(0, 0): tops(k, depth + ahead)}
        vols = [jnp.where(sub == middle, fields[k][1], zero), zero]
        for a in range(-deepest, deepest + 1):
            if (a, 0) in around and around[a, 0] <= depth:
                got = taken((a, 0))
                pots[a, 0] = got[0]
                vols[0] = jnp.where(sub == middle + a, got[1], vols[0])
                levels[a, 0] = got[2:]
            if (a, 1) in around and around[a, 1] <= depth:
                got = {b: taken((a, b)) for b in (-1, 1)}
                got = beside(got, slots, 2 + depth - around[a, 1])
                pots[a, 1] = got[0]
                vols[1] = jnp.where(sub == middle + a, got[1], vols[1])
                levels[a, 1] = got[2:]
        if phase == 0:
            fixed = {(0, 0): (exch, slope, diff)}
            exists = {(0, 0): 1.0}
            exist_vols = [jnp.where(sub == middle, 1.0, zero), zero]
            for a in range(-deepest, deepest + 1):
                if (a, 0) in around and around[a, 0] < deepest:
                    kinds = (1, 2, 0) if around[a, 0] <= deepest - 2 else (1, 2)
                    fixed[a, 0] = tuple(
                        jnp.where(there[a, 0], halos[0, place[a, 0], i], 0.0) for i in kinds
                    )
                    exists[a, 0] = jnp.where(there[a, 0], 1.0, zero)
                    exist_vols[0] = jnp.where(sub == middle + a, exists[a, 0], exist_vols[0])
                if (a, 1) in around and around[a, 1] < deepest:
                    number = 3 if around[a, 1] <= deepest - 2 else 2
                    got = {
                        b: [jnp.where(there[a, b], halos[0, place[a, b], 0], 0.0)]
                        for b in (-1, 1)
                    }
                    fixed[a, 1] = tuple(beside(got, fixed_slots, number))
                    exists[a, 1] = jnp.where(
                        cell_y < cy // 2,
                        jnp.where(there[a, 1], 1.0, zero),
                        jnp.where(there[a, -1], 1.0, zero),
                    )
                    exist_vols[1] = jnp.where(sub == middle + a, exists[a, 1], exist_vols[1])
        before = {o: None for o in levels}
        past_pots, past_vols = {}, [None, None]
        currents = []
        for step in range(depth):
            terms = recurrence[k + step]
            reach = depth - step - 1
            todo = [o for o in pots if o == (0, 0) or around[o] <= reach]
            rolled = {}

            def rolled_pots(o, shift):
                if o not in pots:
                    return zero
                if (o, shift) not in rolled:
                    rolled[o, shift] = roll(pots[o], shift)
                return rolled[o, shift]

            def rolled_vols(b, shift):
                if ("v", b, shift) not in rolled:
                    rolled["v", b, shift] = roll(vols[b], shift)
                return rolled["v", b, shift]

            wide = (cx - 1) * cy
            new_pots, new_levels, sums = {}, {}, [zero, zero]
            for o in todo:
                a, b = o
                p = pots[o]
                across = jnp.where(
                    low_x, rolled_pots((a - 1, b), -wide), rolled_pots(o, cy)
                ) + jnp.where(high_x, rolled_pots((a + 1, b), wide), rolled_pots(o, -cy))
                other = (a, 1 - b)
                along = jnp.where(
                    low_y, rolled_pots(other, 1 - cy), rolled_pots(o, 1)
                ) + jnp.where(high_y, rolled_pots(other, cy - 1), rolled_pots(o, -1))
                near_vol = jnp.broadcast_to(
                    vols[b][middle + a : middle + a + 1, :], (subs, LANES)
                )
                current = fixed[o][0] * (p - near_vol)
                total = current
                shift = subs // 2
                while shift:
                    total = total + roll(total, shift, 0)
                    shift //= 2
                sums[b] = jnp.where(sub == middle + a, total, sums[b])
                image = (
                    node_cond * node_mirror(p)
                    + current
                    - fixed[o][1] * levels[o][0]
                    + plane_cond * (4.0 * p - (across + along))
                )
                value = relate(image, p, past_pots.get(o), terms)
                if o == (0, 0):
                    currents.append(current)
                else:
                    value = value * exists[o]
                new_pots[o] = value
                new_levels[o] = (
                    shell_images(levels[o], before[o], current, fixed[o][2], terms)
                    if len(levels[o]) > 1
                    else []
                )
            new_vols = []
            for b in range(2):
                across = jnp.where(
                    low_x, roll(rolled_vols(b, -wide), 1, 0), rolled_vols(b, cy)
                ) + jnp.where(high_x, roll(rolled_vols(b, wide), -1, 0), rolled_vols(b, -cy))
                along = jnp.where(
                    low_y, rolled_vols(1 - b, 1 - cy), rolled_vols(b, 1)
                ) + jnp.where(high_y, rolled_vols(1 - b, cy - 1), rolled_vols(b, -1))
                mean = add([sums[b]] + [roll(sums[b], g * cells) for g in range(1, groups)])
                image = collector_cond * (4.0 * vols[b] - (across + along)) - mean * (1.0 / nodes)
                new_vols.append(relate(image, vols[b], past_vols[b], terms) * exist_vols[b])
            past_pots, past_vols, before = pots, vols, levels
            pots, vols, levels = new_pots, new_vols, new_levels
            fields[k + step + 1] = (
                pots[0, 0],
                jnp.broadcast_to(vols[0][middle : middle + 1, :], (subs, LANES)),
            )
        if more:
            send_edges(phase + 1, fields[k + depth], levels[0, 0])
        for step in range(depth):
            if k + step not in imaged:
                products += image_shells(
                    k + step, currents[step], recurrence[k + step], not more
                )
            products_pots = pots_products(k + step, fields)
            base = len(products) - len(products_pots)
            products[base:] = [c + o for c, o in zip(products[base:], products_pots)]
        send_row(phase + 1, line_up(products, 0))
        at = len(products)
        if more:
            early_count, early_size = at, k + depth + 1
            products = image_shells(
                k + depth,
                exch * (fields[k + depth][0] - fields[k + depth][1]),
                restart,
            )
            imaged = {k + depth}
        k += depth
    bases = [r[:3] for r in recurrence]
    upper, inverse, images, vectors = [], [], [], []
    target, cosines, sines, uppers = [], [], [], []

    assert len(PLAN) == 2

    def solve_columns(first, last, gram):
        for j in range(first, last):
            factor_column(gram, upper, inverse)
            if j == 0:
                height = jnp.sqrt(gram[0][0] + epsilon)
                target.append(height)
                vectors.append([upper[0][0] / height])
            else:
                project_column(upper, inverse, bases, images)
                entries = arnoldi_column(images, vectors)
                rotate_column(entries, target, cosines, sines, uppers)

    early += take_row(1, early_count)
    gram = symmetric(early, early_size)
    solve_columns(0, early_size, gram)
    gram = symmetric(early + take_row(len(PLAN), at), ITERS + 1)
    solve_columns(early_size, ITERS + 1, gram)
    weights = expand(back_substitute(target, uppers), vectors, upper, inverse)

    sol_p = add([w * f[0] for w, f in zip(weights, fields)])
    sol_v = add([w * f[1] for w, f in zip(weights, fields)])

    mixed = [
        add([weights[i][None] * basis[i, pl.ds(c * CHUNK + 1, CHUNK)] for i in range(ITERS)])
        for c in range(shells // CHUNK)
    ]
    mixed = jnp.concatenate(mixed, axis=0)
    flat = jnp.concatenate([mixed[:, s, :] for s in range(subs)], axis=0)
    sol_turned_ref[...] = flat.T
    flat_p = jnp.concatenate(
        [sol_p[:, g * cells : (g + 1) * cells] for g in range(groups)] + [sol_v[:1, :cells]], axis=0
    )
    sol_pots_ref[...] = flat_p.T.reshape(cx, cy, nodes + 1)

    for phase in range(len(PLAN)):
        for o, copy in copies_of(phase):
            pl.when(there[o])(copy.wait_send)
    for step in range(len(PLAN) + 1):
        part = rows.at[step, pl.ds(0, count - 1)]
        pltpu.make_async_copy(part, part, row_send.at[step]).wait()


def place_outputs(flat_ref, pots_ref, sol_conc_ref, sol_pots_ref, conc_sem, pots_sem):
    cx, cy = sol_conc_ref.shape[0], sol_conc_ref.shape[1]
    cells = cx * cy
    groups = LANES // cells
    span = flat_ref.shape[1]
    copies = [pltpu.make_async_copy(pots_ref, sol_pots_ref, pots_sem)]
    for x in range(cx):
        for g in range(groups):
            edge_row = g * cells + x * cy
            copies.append(
                pltpu.make_async_copy(
                    flat_ref.at[edge_row : edge_row + cy, :],
                    sol_conc_ref.at[x, :, g * span : (g + 1) * span],
                    conc_sem.at[x, g],
                )
            )
    for copy in copies:
        copy.start()
    for copy in copies:
        copy.wait()


def solution(mesh):
    sizes = (mesh.shape["gx"], mesh.shape["gy"])
    count = sizes[0] * sizes[1]

    def shards(rhs_conc, rhs_pots, diffusion, exchange, slope):
        cx, cy = rhs_conc.shape[0], rhs_conc.shape[1]
        cells = cx * cy
        nodes = exchange.shape[2]
        shells = rhs_conc.shape[2] // nodes
        groups = LANES // cells
        subs = nodes // groups
        deepest = max(PLAN)
        near = len(surroundings(cx, cy, deepest))
        phases = len(PLAN)
        widest = strip_slots(phase_widths(deepest), cy)
        pages = pages_of(widest, len(widest))
        vmem = pl.BlockSpec(memory_space=pltpu.VMEM)
        anywhere = pl.BlockSpec(memory_space=pl.ANY)
        dma = pltpu.SemaphoreType.DMA
        inputs = [
            pltpu.with_memory_space_constraint(x, pltpu.HBM)
            for x in (rhs_conc, rhs_pots, diffusion, exchange, slope)
        ]
        flat, sol_pots = pl.pallas_call(
            functools.partial(cycle, sizes),
            out_shape=(
                jax.ShapeDtypeStruct((LANES, subs * shells), jnp.float32),
                jax.ShapeDtypeStruct(rhs_pots.shape, jnp.float32),
            ),
            in_specs=[anywhere] * 5,
            out_specs=(vmem, vmem),
            scratch_shapes=[
                pltpu.VMEM((LANES, subs * shells), jnp.float32),
                pltpu.VMEM((ITERS + 1, shells + 2, subs, LANES), jnp.float32),
                pltpu.VMEM(rhs_pots.shape, jnp.float32),
                pltpu.VMEM((3,) + exchange.shape, jnp.float32),
                pltpu.VMEM((phases, deepest + 4, subs, LANES), jnp.float32),
                pltpu.VMEM((phases, 2, pages + 1, subs, LANES), jnp.float32),
                pltpu.VMEM((phases, near, deepest + 4, subs, LANES), jnp.float32),
                pltpu.VMEM((phases + 1, count, 1, LANES), jnp.float32),
                pltpu.VMEM((phases + 1, 1, LANES), jnp.float32),
                dma((phases, near)),
                dma((phases, near)),
                dma((phases + 1,)),
                dma((phases + 1,)),
                dma((cx, groups)),
                dma((4,)),
            ],
            compiler_params=pltpu.CompilerParams(
                collective_id=0,
                has_side_effects=True,
                vmem_limit_bytes=12 * 1024 * 1024,
            ),
        )(*inputs)
        return pl.pallas_call(
            place_outputs,
            out_shape=(
                jax.ShapeDtypeStruct(rhs_conc.shape, jnp.float32),
                jax.ShapeDtypeStruct(rhs_pots.shape, jnp.float32),
            ),
            in_specs=[vmem, vmem],
            out_specs=(anywhere, anywhere),
            scratch_shapes=[dma((cx, groups)), dma],
            compiler_params=pltpu.CompilerParams(vmem_limit_bytes=12 * 1024 * 1024),
        )(flat, sol_pots)

    spec = P("gx", "gy", None)
    return jax.shard_map(
        shards,
        mesh=mesh,
        in_specs=(spec,) * 5,
        out_specs=(spec, spec),
        check_vma=False,
    )
```

```python
import functools

import jax
import jax.numpy as jnp
from jax import lax
from jax.experimental import pallas as pl
from jax.experimental.pallas import tpu as pltpu
from jax.sharding import PartitionSpec as P

ITERS = 10
LANES = 128
CHUNK = 32
PLAN = (5, 5)
ADAPTIVE = 2

node_cond = 1.0
plane_cond = 0.5
collector_cond = 2.0
epsilon = 1e-06
center = 10.0
radius = 10.0
least_height = 0.05
least_pivot = 3e-07
MESH = pl.DeviceIdType.MESH


def add(terms):
    terms = [t for t in terms if t is not None]
    while len(terms) > 1:
        pairs = [terms[k] + terms[k + 1] for k in range(0, len(terms) - 1, 2)]
        terms = pairs + ([terms[-1]] if len(terms) % 2 else [])
    return terms[0]


def factor_column(gram, upper, inverse):
    j = len(inverse)
    column = []
    for i in range(j):
        value = gram[i][j]
        if i:
            value = value - add([upper[i][m] * column[m] for m in range(i)])
        column.append(value * inverse[i])
    pivot = gram[j][j]
    if j:
        pivot = pivot - add([c * c for c in column])
    good = pivot > least_pivot * gram[j][j]
    inv = jnp.where(good, lax.rsqrt(jnp.where(good, pivot, 1.0)), 0.0)
    upper.append(column + [pivot * inv])
    inverse.append(inv)


def project_column(upper, inverse, recurrence, columns):
    k = len(columns)
    alpha, gamma, beta = recurrence[k]
    column = []
    for i in range(k + 2):
        terms = [beta * upper[k + 1][i]]
        if i <= k:
            terms.append(alpha * upper[k][i])
        if i <= k - 1 and gamma is not None:
            terms.append(gamma * upper[k - 1][i])
        value = add(terms)
        known = [columns[m][i] * upper[k][m] for m in range(max(i - 1, 0), k)]
        if known:
            value = value - add(known)
        column.append(value * inverse[k])
    columns.append(column)


def arnoldi_column(images, vectors):
    j = len(vectors) - 1
    newest = vectors[j]
    image = [
        add([images[k][t] * newest[k] for k in range(max(t - 1, 0), j + 1)]) for t in range(j + 2)
    ]
    coeffs = [add([vectors[i][t] * image[t] for t in range(i + 1)]) for i in range(j + 1)]
    rest = [
        image[t] - add([coeffs[i] * vectors[i][t] for i in range(t, j + 1)]) for t in range(j + 1)
    ] + [image[j + 1]]
    square = add([r * r for r in rest]) + epsilon
    scale = lax.rsqrt(square)
    height = square * scale
    vectors.append([r * scale for r in rest])
    return coeffs + [height]


def rotate_column(entries, target, cosines, sines, uppers):
    step = len(uppers)
    entries = list(entries)
    for row in range(step):
        first = cosines[row] * entries[row] + sines[row] * entries[row + 1]
        second = cosines[row] * entries[row + 1] - sines[row] * entries[row]
        entries[row] = first
        entries[row + 1] = second
    square = entries[step] * entries[step] + entries[step + 1] * entries[step + 1]
    shrink = lax.rsqrt(square)
    size = square * shrink
    cosine = entries[step] * shrink
    sine = entries[step + 1] * shrink
    entries[step] = size
    cosines.append(cosine)
    sines.append(sine)
    lead = target[step]
    target[step] = cosine * lead
    target.append(-sine * lead)
    uppers.append((entries[: step + 1], shrink))


def back_substitute(target, uppers):
    count = len(uppers)
    weights = [None] * count
    for row in range(count - 1, -1, -1):
        total = target[row]
        for later in range(count - 1, row, -1):
            total = total - uppers[later][0][row] * weights[later]
        weights[row] = total * uppers[row][1]
    return weights


def expand(weights, vectors, upper, inverse):
    count = len(weights)
    along = [add([vectors[j][t] * weights[j] for j in range(t, count)]) for t in range(count)]
    out = [None] * count
    for row in range(count - 1, -1, -1):
        total = along[row]
        for later in range(count - 1, row, -1):
            total = total - upper[later][row] * out[later]
        out[row] = total * inverse[row]
    return out


def surroundings(cx, cy, depth):
    def away(extent, offset):
        return (abs(offset) - 1) * extent + 1 if offset else 0

    found = {}
    for a in range(-depth, depth + 1):
        for b in range(-depth, depth + 1):
            distance = away(cx, a) + away(cy, b)
            if 0 < distance <= depth:
                found[a, b] = distance
    return found


def strip_slots(widths, room):
    out, page, at = [], 0, 0
    for width in widths:
        if at + width > room:
            page, at = page + 1, 0
        out.append((page, at, width))
        at += width
    return out


def phase_widths(depth):
    return [depth, depth] + list(range(depth - 1, 0, -1))


def pages_of(slots, number):
    return 1 + max(page for page, _, _ in slots[:number])


def cycle(
    sizes,
    conc_ref,
    pots_ref,
    diff_ref,
    exch_ref,
    slope_ref,
    sol_turned_ref,
    sol_pots_ref,
    turned,
    basis,
    raw_pots,
    raw_fixed,
    sent,
    strips,
    halos,
    rows,
    sent_rows,
    edge_send,
    edge_recv,
    row_send,
    row_recv,
    load_sem,
    small_sem,
):
    nx, ny = sizes
    count = nx * ny
    cx, cy = conc_ref.shape[0], conc_ref.shape[1]
    cells = cx * cy
    nodes = exch_ref.shape[2]
    shells = conc_ref.shape[2] // nodes
    groups = LANES // cells
    subs = nodes // groups
    mx = lax.axis_index("gx")
    my = lax.axis_index("gy")
    me = mx * ny + my
    deepest = max(PLAN)
    around = surroundings(cx, cy, deepest)
    order = sorted(around, key=lambda o: -around[o])
    place = {o: i for i, o in enumerate(order)}

    def peers(act):
        if count <= 32:
            for dx in range(nx - 1, -1, -1):
                for dy in range(ny - 1, -1, -1):
                    if dx or dy:
                        act(lax.rem(mx + dx, nx), lax.rem(my + dy, ny))
        else:

            def one(p, carry):
                other = lax.rem(me + p, count)
                act(lax.div(other, ny), lax.rem(other, ny))
                return carry

            lax.fori_loop(1, count, one, 0)

    barrier = pltpu.get_barrier_semaphore()
    peers(
        lambda px, py: pl.semaphore_signal(
            barrier, inc=1, device_id={"gx": px, "gy": py}, device_id_type=MESH
        )
    )

    span = subs * shells
    loads = []
    for x in range(cx):
        for g in range(groups):
            edge_row = g * cells + x * cy
            loads.append(
                pltpu.make_async_copy(
                    conc_ref.at[x, :, g * span : (g + 1) * span],
                    turned.at[edge_row : edge_row + cy, :],
                    load_sem.at[x, g],
                )
            )
    small = [pltpu.make_async_copy(pots_ref, raw_pots, small_sem.at[0])]
    for k, ref in enumerate((exch_ref, slope_ref, diff_ref)):
        small.append(pltpu.make_async_copy(ref, raw_fixed.at[k], small_sem.at[k + 1]))
    for copy in small + loads:
        copy.start()
    for copy in small:
        copy.wait()

    def fold_nodes(block):
        return block.reshape(cells, block.shape[2]).T

    def node_register(flat_t):
        return jnp.concatenate(
            [flat_t[g * subs : (g + 1) * subs, :] for g in range(groups)], axis=1
        )

    exch = node_register(fold_nodes(raw_fixed[0]))
    slope = node_register(fold_nodes(raw_fixed[1]))
    diff = node_register(fold_nodes(raw_fixed[2]))
    pots_t = fold_nodes(raw_pots[...])
    pot = node_register(pots_t)
    vol_row = pots_t[nodes : nodes + 1, :]
    vol = jnp.broadcast_to(jnp.concatenate([vol_row] * groups, axis=1), (subs, LANES))

    lane = lax.broadcasted_iota(jnp.int32, (subs, LANES), 1)
    sub = lax.broadcasted_iota(jnp.int32, (subs, LANES), 0)
    group = lane // cells
    cell = lane % cells
    cell_x = cell // cy
    cell_y = cell % cy
    single = ((sub == 0) & (group == 0)).astype(jnp.float32)
    first_sub, last_sub = sub == 0, sub == subs - 1
    first_group, last_group = group == 0, group == groups - 1
    low_x, high_x = cell_x == 0, cell_x == cx - 1
    low_y, high_y = cell_y == 0, cell_y == cy - 1
    zero = jnp.zeros((subs, LANES), jnp.float32)
    middle = (subs - 1) // 2

    there = {}
    for a, b in order:
        there[a, b] = (
            (mx + a >= 0) & (mx + a < nx) & (my + b >= 0) & (my + b < ny)
        )

    def roll(value, shift, axis=1):
        shift = shift % value.shape[axis]
        return pltpu.roll(value, shift, axis) if shift else value

    def pack(values, slots, to_low):
        packed = [zero] * pages_of(slots, len(slots))
        for value, (page, at, width) in zip(values, slots):
            if to_low:
                held = (cell_y >= at) & (cell_y < at + width)
                packed[page] = jnp.where(held, roll(value, at), packed[page])
            else:
                held = (cell_y >= cy - at - width) & (cell_y < cy - at)
                packed[page] = jnp.where(held, roll(value, -at), packed[page])
        return packed

    def unpack(pages, slot, from_high):
        page, at, width = slot
        packed = pages[page]
        if from_high:
            return jnp.where(cell_y < width, roll(packed, -at), zero)
        return jnp.where(cell_y >= cy - width, roll(packed, at), zero)

    def phase_slots(phase):
        return strip_slots(phase_widths(PLAN[phase]), cy)

    fixed_slots = strip_slots([deepest - 1, deepest - 1, max(deepest - 2, 0)], cy)

    def items_of(phase, o):
        number = 2 + PLAN[phase] - around[o]
        return pages_of(phase_slots(phase), number) if o[1] else number

    def first_of(phase, o):
        if phase:
            return 0
        if o[1]:
            return 0 if around[o] < deepest else 1
        return {0: 3, 1: 1}.get(deepest - around[o], 0)

    def offset_of(phase, b):
        return 0 if phase else 1 if b else 3

    def sides(p, low_block, high_block, edge_low, edge_high, step, wide):
        low = roll(p, step)
        low = jnp.where(edge_low, zero if low_block is None else roll(low_block, -wide), low)
        high = roll(p, -step)
        high = jnp.where(edge_high, zero if high_block is None else roll(high_block, wide), high)
        return low + high

    def plane(p, near, member):
        def at(offset):
            return None if near[offset] is None else near[offset][member]

        across = sides(p, at((-1, 0)), at((1, 0)), low_x, high_x, cy, (cx - 1) * cy)
        along = sides(p, at((0, -1)), at((0, 1)), low_y, high_y, 1, cy - 1)
        return 4.0 * p - (across + along)

    def node_mirror(p):
        low = roll(p, 1, 0)
        inner = jnp.where(first_sub, jnp.where(first_group, p, roll(low, cells)), low)
        high = roll(p, -1, 0)
        outer = jnp.where(last_sub, jnp.where(last_group, p, roll(high, -cells)), high)
        return 2.0 * p - inner - outer

    def node_mean(value):
        total = jnp.broadcast_to(jnp.sum(value, axis=0, keepdims=True), (subs, LANES))
        parts = [total] + [roll(total, g * cells) for g in range(1, groups)]
        return add(parts) * (1.0 / nodes)

    nowhere = {(-1, 0): None, (1, 0): None, (0, -1): None, (0, 1): None}

    def pots_image(field, near, surface, fixed):
        p, v = field
        current = fixed[0] * (p - v)
        new_p = (
            node_cond * node_mirror(p)
            + current
            - fixed[1] * surface
            + plane_cond * plane(p, near, 0)
        )
        new_v = collector_cond * plane(v, near, 1) - node_mean(current)
        return new_p, new_v, current

    def relate(image, here, before, terms):
        alpha, gamma, _, inverse = terms
        value = image - alpha * here
        if gamma is not None:
            value = value - gamma * before
        return value * inverse

    def shell_images(levels, before, current, diffusion, terms):
        out = []
        for k in range(len(levels) - 1):
            here = levels[k]
            image = here + diffusion * (
                here - levels[k + 1] if k == 0 else 2.0 * here - levels[k - 1] - levels[k + 1]
            )
            if k == 0:
                image = image + current
            out.append(relate(image, here, before[k] if before else None, terms))
        return out

    def pots_products(k, fields):
        newest = fields[k + 1]
        return [
            fields[i][0] * newest[0] + fields[i][1] * (newest[1] * single) for i in range(k + 2)
        ]

    def image_shells(k, current, terms, straight=False):
        alpha, gamma, _, inverse = terms
        keep = (1.0 - alpha) * inverse
        spread = diff * inverse
        middle_part = (keep + 2.0 * spread)[None]
        spread = spread[None]
        basis[k, 0] = basis[k, 1]
        basis[k, shells + 1] = basis[k, shells]
        pushed = inverse * current
        drag = None if gamma is None else gamma * inverse

        def part(at, carry, last):
            here = basis[k, pl.ds(at + 1, CHUNK)]
            low = basis[k, pl.ds(at, CHUNK)]
            high = basis[k, pl.ds(at + 2, CHUNK)]
            new = middle_part * here - spread * (low + high)
            others = [basis[i, pl.ds(at + 1, CHUNK)] for i in range(k)] + [here]
            if drag is not None:
                behind = others[k - 1]
                new = new - (behind if isinstance(drag, float) and drag == 1.0 else drag * behind)
            if last:
                new = jnp.concatenate([new[:-1], new[-1:] + pushed[None]], axis=0)
            basis[k + 1, pl.ds(at + 1, CHUNK)] = new
            return tuple(
                c + jnp.sum(o * new, axis=0) for c, o in zip(carry, others + [new])
            )

        parts = shells // CHUNK
        if straight:
            carry = (zero,) * (k + 2)
            for c in range(parts - 1):
                carry = part(c * CHUNK, carry, False)
            return list(part((parts - 1) * CHUNK, carry, True))
        carry = lax.fori_loop(
            0,
            parts - 1,
            lambda c, carry: part(c * CHUNK, carry, False),
            (zero,) * (k + 2),
        )
        return list(part((parts - 1) * CHUNK, carry, True))

    def line_up(products, offset):
        padded = -(-len(products) // 8) * 8
        stacked = [jnp.sum(d, axis=0, keepdims=True) for d in products]
        stacked += [zero[:1]] * (padded - len(products))
        tall = jnp.sum(jnp.concatenate(stacked, axis=0), axis=1, keepdims=True)
        at_row = lax.broadcasted_iota(jnp.int32, (padded, LANES), 0) + offset
        at_lane = lax.broadcasted_iota(jnp.int32, (padded, LANES), 1)
        return jnp.sum(jnp.where(at_row == at_lane, tall, 0.0), axis=0, keepdims=True)

    def row_copy(step, px, py):
        return pltpu.make_async_remote_copy(
            src_ref=sent_rows.at[step],
            dst_ref=rows.at[step, me],
            send_sem=row_send.at[step],
            recv_sem=row_recv.at[step],
            device_id={"gx": px, "gy": py},
            device_id_type=MESH,
        )

    def send_row_only(step):
        peers(lambda px, py: row_copy(step, px, py).start())

    def send_row(step, row):
        sent_rows[step] = row
        rows[step, me] = row
        send_row_only(step)

    def take_row(step, wanted):
        part = rows.at[step, pl.ds(0, count - 1)]
        pltpu.make_async_copy(part, part, row_recv.at[step]).wait()
        total = jnp.sum(rows[step], axis=0)
        return [jnp.broadcast_to(total[:, k : k + 1], (subs, LANES)) for k in range(wanted)]

    def copies_of(phase):
        depth = PLAN[phase]
        out = []
        for o in order:
            if around[o] > depth:
                continue
            a, b = o
            start = first_of(phase, o)
            items = offset_of(phase, b) + items_of(phase, o) - start
            out.append(
                (
                    o,
                    pltpu.make_async_remote_copy(
                        src_ref=strips.at[phase, (b + 1) // 2, pl.ds(start, items)]
                        if b
                        else sent.at[phase, pl.ds(start, items)],
                        dst_ref=halos.at[phase, place[-a, -b], pl.ds(start, items)],
                        send_sem=edge_send.at[phase, place[o]],
                        recv_sem=edge_recv.at[phase, place[-a, -b]],
                        device_id={
                            "gx": lax.rem(mx + a + nx * deepest, nx),
                            "gy": lax.rem(my + b + ny * deepest, ny),
                        },
                        device_id_type=MESH,
                    ),
                )
            )
        return out

    def arrivals_of(phase):
        depth = PLAN[phase]
        out = []
        for o in order:
            if around[o] > depth:
                continue
            start = first_of(phase, o)
            items = offset_of(phase, o[1]) + items_of(phase, o) - start
            part = halos.at[phase, place[o], pl.ds(start, items)]
            out.append((o, pltpu.make_async_copy(part, part, edge_recv.at[phase, place[o]])))
        return out

    def start_edges(phase):
        for o, copy in copies_of(phase):
            pl.when(there[o])(copy.start)

    def store_edges(phase, field, levels):
        values = [field[0], field[1]] + list(levels)
        for k, value in enumerate(values):
            sent[phase, offset_of(phase, 0) + k] = value
        for k in range(2):
            for page, packed in enumerate(pack(values, phase_slots(phase), k == 0)):
                strips[phase, k, offset_of(phase, 1) + page] = packed

    def send_edges(phase, field, levels):
        store_edges(phase, field, levels)
        start_edges(phase)

    def tops(k, number):
        return [basis[k, shells - j] for j in range(number)]

    for copy in loads:
        copy.wait()
    turned_t = turned[...].T.reshape(subs, shells, LANES)
    for s in range(subs):
        basis[0, 1 : shells + 1, s, :] = turned_t[s]

    fields = [(pot, vol)] + [None] * ITERS
    fixed_own = (exch, slope)
    guess = [(center, None, radius, 1.0 / radius), (center, radius / 2, radius / 2, 2.0 / radius)]

    local = [fields[0]]
    products = [
        pot * pot
        + vol * (vol * single)
        + lax.fori_loop(
            0,
            shells // CHUNK,
            lambda c, t: t
            + jnp.sum(
                basis[0, pl.ds(c * CHUNK + 1, CHUNK)] * basis[0, pl.ds(c * CHUNK + 1, CHUNK)],
                axis=0,
            ),
            zero,
        )
    ]
    first_square = products[0]
    for k in range(ADAPTIVE):
        new_p, new_v, current = pots_image(local[k], nowhere, basis[k, shells], fixed_own)
        before = local[k - 1] if k else (None, None)
        local.append(
            (
                relate(new_p, local[k][0], before[0], guess[k]),
                relate(new_v, local[k][1], before[1], guess[k]),
            )
        )
        inner = image_shells(k, current, guess[k])
        products += [c + o for c, o in zip(inner, pots_products(k, local))]
    local_row = line_up(products, 0)
    local_count = len(products)
    store_edges(0, fields[0], tops(0, PLAN[0] - 1))
    for k, value in enumerate((diff, exch, slope)):
        sent[0, k] = value
    for k in range(2):
        strips[0, k, 0] = pack((exch, slope, diff), fixed_slots, k == 0)[0]
    sent_rows[0] = local_row
    rows[0, me] = local_row
    pl.semaphore_wait(barrier, count - 1)
    start_edges(0)
    send_row_only(0)

    def symmetric(sums, size):
        gram = [[None] * size for _ in range(size)]
        at = 0
        for j in range(size):
            for i in range(j + 1):
                gram[i][j] = gram[j][i] = sums[at]
                at += 1
        return gram

    def lanczos(sums):
        gram = symmetric(sums, ADAPTIVE + 1)
        upper, inverse, columns = [], [], []
        for k in range(ADAPTIVE + 1):
            factor_column(gram, upper, inverse)
            if k:
                project_column(upper, inverse, [g[:3] for g in guess], columns)
        out = []
        for k in range(ADAPTIVE):
            height = jnp.maximum(columns[k][k + 1], least_height)
            gamma = columns[k][k - 1] if k else None
            out.append((columns[k][k], gamma, height, 1.0 / height))
        return out

    recurrence = None
    restart = (center, None, radius, 1.0 / radius)
    usual = (center, radius / 2, radius / 2, 2.0 / radius)
    products = [first_square]
    imaged = set()
    early = []
    k = 0
    for phase, depth in enumerate(PLAN):
        more = phase + 1 < len(PLAN)
        ahead = PLAN[phase + 1] - 1 if more else 0
        if phase == 0:
            recurrence = lanczos(take_row(0, local_count))
        for step in range(depth):
            if k + step < ADAPTIVE:
                continue
            recurrence.append(usual if step else restart)
        for o, copy in arrivals_of(phase):
            pl.when(there[o])(copy.wait)
        slots = phase_slots(phase)

        def taken(o):
            return [
                jnp.where(there[o], halos[phase, place[o], offset_of(phase, o[1]) + i], 0.0)
                for i in range(items_of(phase, o))
            ]

        def beside(got, page_slots, number):
            return [
                add([unpack(got[b], page_slots[i], b > 0) for b in got]) for i in range(number)
            ]

        pots = {(0, 0): fields[k][0]}
        levels = {(0, 0): tops(k, depth + ahead)}
        vols = [jnp.where(sub == middle, fields[k][1], zero), zero]
        for a in range(-deepest, deepest + 1):
            if (a, 0) in around and around[a, 0] <= depth:
                got = taken((a, 0))
                pots[a, 0] = got[0]
                vols[0] = jnp.where(sub == middle + a, got[1], vols[0])
                levels[a, 0] = got[2:]
            if (a, 1) in around and around[a, 1] <= depth:
                got = {b: taken((a, b)) for b in (-1, 1)}
                got = beside(got, slots, 2 + depth - around[a, 1])
                pots[a, 1] = got[0]
                vols[1] = jnp.where(sub == middle + a, got[1], vols[1])
                levels[a, 1] = got[2:]
        if phase == 0:
            fixed = {(0, 0): (exch, slope, diff)}
            exists = {(0, 0): 1.0}
            exist_vols = [jnp.where(sub == middle, 1.0, zero), zero]
            for a in range(-deepest, deepest + 1):
                if (a, 0) in around and around[a, 0] < deepest:
                    kinds = (1, 2, 0) if around[a, 0] <= deepest - 2 else (1, 2)
                    fixed[a, 0] = tuple(
                        jnp.where(there[a, 0], halos[0, place[a, 0], i], 0.0) for i in kinds
                    )
                    exists[a, 0] = jnp.where(there[a, 0], 1.0, zero)
                    exist_vols[0] = jnp.where(sub == middle + a, exists[a, 0], exist_vols[0])
                if (a, 1) in around and around[a, 1] < deepest:
                    number = 3 if around[a, 1] <= deepest - 2 else 2
                    got = {
                        b: [jnp.where(there[a, b], halos[0, place[a, b], 0], 0.0)]
                        for b in (-1, 1)
                    }
                    fixed[a, 1] = tuple(beside(got, fixed_slots, number))
                    exists[a, 1] = jnp.where(
                        cell_y < cy // 2,
                        jnp.where(there[a, 1], 1.0, zero),
                        jnp.where(there[a, -1], 1.0, zero),
                    )
                    exist_vols[1] = jnp.where(sub == middle + a, exists[a, 1], exist_vols[1])
        before = {o: None for o in levels}
        past_pots, past_vols = {}, [None, None]
        currents = []
        for step in range(depth):
            terms = recurrence[k + step]
            reach = depth - step - 1
            todo = [o for o in pots if o == (0, 0) or around[o] <= reach]
            rolled = {}

            def rolled_pots(o, shift):
                if o not in pots:
                    return zero
                if (o, shift) not in rolled:
                    rolled[o, shift] = roll(pots[o], shift)
                return rolled[o, shift]

            def rolled_vols(b, shift):
                if ("v", b, shift) not in rolled:
                    rolled["v", b, shift] = roll(vols[b], shift)
                return rolled["v", b, shift]

            wide = (cx - 1) * cy
            new_pots, new_levels, sums = {}, {}, [zero, zero]
            for o in todo:
                a, b = o
                p = pots[o]
                across = jnp.where(
                    low_x, rolled_pots((a - 1, b), -wide), rolled_pots(o, cy)
                ) + jnp.where(high_x, rolled_pots((a + 1, b), wide), rolled_pots(o, -cy))
                other = (a, 1 - b)
                along = jnp.where(
                    low_y, rolled_pots(other, 1 - cy), rolled_pots(o, 1)
                ) + jnp.where(high_y, rolled_pots(other, cy - 1), rolled_pots(o, -1))
                near_vol = jnp.broadcast_to(
                    vols[b][middle + a : middle + a + 1, :], (subs, LANES)
                )
                current = fixed[o][0] * (p - near_vol)
                total = current
                shift = subs // 2
                while shift:
                    total = total + roll(total, shift, 0)
                    shift //= 2
                sums[b] = jnp.where(sub == middle + a, total, sums[b])
                image = (
                    node_cond * node_mirror(p)
                    + current
                    - fixed[o][1] * levels[o][0]
                    + plane_cond * (4.0 * p - (across + along))
                )
                value = relate(image, p, past_pots.get(o), terms)
                if o == (0, 0):
                    currents.append(current)
                else:
                    value = value * exists[o]
                new_pots[o] = value
                new_levels[o] = (
                    shell_images(levels[o], before[o], current, fixed[o][2], terms)
                    if len(levels[o]) > 1
                    else []
                )
            new_vols = []
            for b in range(2):
                across = jnp.where(
                    low_x, roll(rolled_vols(b, -wide), 1, 0), rolled_vols(b, cy)
                ) + jnp.where(high_x, roll(rolled_vols(b, wide), -1, 0), rolled_vols(b, -cy))
                along = jnp.where(
                    low_y, rolled_vols(1 - b, 1 - cy), rolled_vols(b, 1)
                ) + jnp.where(high_y, rolled_vols(1 - b, cy - 1), rolled_vols(b, -1))
                mean = add([sums[b]] + [roll(sums[b], g * cells) for g in range(1, groups)])
                image = collector_cond * (4.0 * vols[b] - (across + along)) - mean * (1.0 / nodes)
                new_vols.append(relate(image, vols[b], past_vols[b], terms) * exist_vols[b])
            past_pots, past_vols, before = pots, vols, levels
            pots, vols, levels = new_pots, new_vols, new_levels
            fields[k + step + 1] = (
                pots[0, 0],
                jnp.broadcast_to(vols[0][middle : middle + 1, :], (subs, LANES)),
            )
        if more:
            send_edges(phase + 1, fields[k + depth], levels[0, 0])
        for step in range(depth):
            if k + step not in imaged:
                products += image_shells(
                    k + step, currents[step], recurrence[k + step], not more
                )
            products_pots = pots_products(k + step, fields)
            base = len(products) - len(products_pots)
            products[base:] = [c + o for c, o in zip(products[base:], products_pots)]
        send_row(phase + 1, line_up(products, 0))
        at = len(products)
        if more:
            early_count, early_size = at, k + depth + 1
            products = image_shells(
                k + depth,
                exch * (fields[k + depth][0] - fields[k + depth][1]),
                restart,
            )
            imaged = {k + depth}
        k += depth
    bases = [r[:3] for r in recurrence]
    upper, inverse, images, vectors = [], [], [], []
    target, cosines, sines, uppers = [], [], [], []

    assert len(PLAN) == 2

    def solve_columns(first, last, gram):
        for j in range(first, last):
            factor_column(gram, upper, inverse)
            if j == 0:
                height = jnp.sqrt(gram[0][0] + epsilon)
                target.append(height)
                vectors.append([upper[0][0] / height])
            else:
                project_column(upper, inverse, bases, images)
                entries = arnoldi_column(images, vectors)
                rotate_column(entries, target, cosines, sines, uppers)

    early += take_row(1, early_count)
    gram = symmetric(early, early_size)
    solve_columns(0, early_size, gram)
    gram = symmetric(early + take_row(len(PLAN), at), ITERS + 1)
    solve_columns(early_size, ITERS + 1, gram)
    weights = expand(back_substitute(target, uppers), vectors, upper, inverse)

    sol_p = add([w * f[0] for w, f in zip(weights, fields)])
    sol_v = add([w * f[1] for w, f in zip(weights, fields)])

    mixed = [
        add([weights[i][None] * basis[i, pl.ds(c * CHUNK + 1, CHUNK)] for i in range(ITERS)])
        for c in range(shells // CHUNK)
    ]
    mixed = jnp.concatenate(mixed, axis=0)
    flat = jnp.concatenate([mixed[:, s, :] for s in range(subs)], axis=0)
    sol_turned_ref[...] = flat.T
    flat_p = jnp.concatenate(
        [sol_p[:, g * cells : (g + 1) * cells] for g in range(groups)] + [sol_v[:1, :cells]], axis=0
    )
    sol_pots_ref[...] = flat_p.T.reshape(cx, cy, nodes + 1)

    for phase in range(len(PLAN)):
        for o, copy in copies_of(phase):
            pl.when(there[o])(copy.wait_send)
    for step in range(len(PLAN) + 1):
        part = rows.at[step, pl.ds(0, count - 1)]
        pltpu.make_async_copy(part, part, row_send.at[step]).wait()


def place_outputs(flat_ref, pots_ref, sol_conc_ref, sol_pots_ref, conc_sem, pots_sem):
    cx, cy = sol_conc_ref.shape[0], sol_conc_ref.shape[1]
    cells = cx * cy
    groups = LANES // cells
    span = flat_ref.shape[1]
    copies = [pltpu.make_async_copy(pots_ref, sol_pots_ref, pots_sem)]
    for x in range(cx):
        for g in range(groups):
            edge_row = g * cells + x * cy
            copies.append(
                pltpu.make_async_copy(
                    flat_ref.at[edge_row : edge_row + cy, :],
                    sol_conc_ref.at[x, :, g * span : (g + 1) * span],
                    conc_sem.at[x, g],
                )
            )
    for copy in copies:
        copy.start()
    for copy in copies:
        copy.wait()


def solution(mesh):
    sizes = (mesh.shape["gx"], mesh.shape["gy"])
    count = sizes[0] * sizes[1]

    def shards(rhs_conc, rhs_pots, diffusion, exchange, slope):
        cx, cy = rhs_conc.shape[0], rhs_conc.shape[1]
        cells = cx * cy
        nodes = exchange.shape[2]
        shells = rhs_conc.shape[2] // nodes
        groups = LANES // cells
        subs = nodes // groups
        deepest = max(PLAN)
        near = len(surroundings(cx, cy, deepest))
        phases = len(PLAN)
        widest = strip_slots(phase_widths(deepest), cy)
        pages = pages_of(widest, len(widest))
        vmem = pl.BlockSpec(memory_space=pltpu.VMEM)
        anywhere = pl.BlockSpec(memory_space=pl.ANY)
        dma = pltpu.SemaphoreType.DMA
        inputs = [
            pltpu.with_memory_space_constraint(x, pltpu.HBM)
            for x in (rhs_conc, rhs_pots, diffusion, exchange, slope)
        ]
        flat, sol_pots = pl.pallas_call(
            functools.partial(cycle, sizes),
            out_shape=(
                jax.ShapeDtypeStruct((LANES, subs * shells), jnp.float32),
                jax.ShapeDtypeStruct(rhs_pots.shape, jnp.float32),
            ),
            in_specs=[anywhere] * 5,
            out_specs=(vmem, vmem),
            scratch_shapes=[
                pltpu.VMEM((LANES, subs * shells), jnp.float32),
                pltpu.VMEM((ITERS + 1, shells + 2, subs, LANES), jnp.float32),
                pltpu.VMEM(rhs_pots.shape, jnp.float32),
                pltpu.VMEM((3,) + exchange.shape, jnp.float32),
                pltpu.VMEM((phases, deepest + 4, subs, LANES), jnp.float32),
                pltpu.VMEM((phases, 2, pages + 1, subs, LANES), jnp.float32),
                pltpu.VMEM((phases, near, deepest + 4, subs, LANES), jnp.float32),
                pltpu.VMEM((phases + 1, count, 1, LANES), jnp.float32),
                pltpu.VMEM((phases + 1, 1, LANES), jnp.float32),
                dma((phases, near)),
                dma((phases, near)),
                dma((phases + 1,)),
                dma((phases + 1,)),
                dma((cx, groups)),
                dma((4,)),
            ],
            compiler_params=pltpu.CompilerParams(
                collective_id=0,
                has_side_effects=True,
                vmem_limit_bytes=12 * 1024 * 1024,
            ),
        )(*inputs)
        return pl.pallas_call(
            place_outputs,
            out_shape=(
                jax.ShapeDtypeStruct(rhs_conc.shape, jnp.float32),
                jax.ShapeDtypeStruct(rhs_pots.shape, jnp.float32),
            ),
            in_specs=[vmem, vmem],
            out_specs=(anywhere, anywhere),
            scratch_shapes=[dma((cx, groups)), dma],
            compiler_params=pltpu.CompilerParams(vmem_limit_bytes=12 * 1024 * 1024),
        )(flat, sol_pots)

    spec = P("gx", "gy", None)
    return jax.shard_map(
        shards,
        mesh=mesh,
        in_specs=(spec,) * 5,
        out_specs=(spec, spec),
        check_vma=False,
    )
```
